32 devices in a mesh: ep: 8 (over z, x), dp: 4 (over y, core).
Axes of the slice: x: 2, y: 2, z: 4, core: 2. Of those that a mesh axis runs over, the one named last changes fastest.
Arguments:
- grad_out: float32 [4096, 1536], P(('ep', 'dp')), may hold values from -6 to 6
- tokens: bfloat16 [4096, 1536], P(('ep', 'dp')), may hold values from -6 to 6
- probs: float32 [4096, 4], P(('ep', 'dp')), may hold values from 0.1 to 0.5
- expert_ids: int32 [4096, 4], P(('ep', 'dp')), may hold values from 0 to 7, all different within a row; in each aligned block of 128 rows (0 to 127, 128 to 255, ...) at most 80 rows name the same one
- priority: int32 [32, 128], P(('ep', 'dp')), may hold values from 0 to 127, each once within a row
- cap_counts: int32 [8], replicated, may hold values from 40 to 80, as said below
- gate_weight: bfloat16 [8, 1536, 1536], P('ep'), may hold values from -0.15625 to 0.15625
- up_weight: bfloat16 [8, 1536, 1536], P('ep'), may hold values from -0.15625 to 0.15625
- down_weight: bfloat16 [8, 1536, 1536], P('ep'), may hold values from -0.15625 to 0.15625
Outputs:
- input_grad: bfloat16 [4096, 1536], P(('ep', 'dp'))
- prob_grad: float32 [4096, 4], P(('ep', 'dp'))
- gate_grad: bfloat16 [8, 1536, 1536], P('ep', 'dp')
- up_grad: bfloat16 [8, 1536, 1536], P('ep', 'dp')
- down_grad: bfloat16 [8, 1536, 1536], P('ep', 'dp')
The draws below stay inside these ranges and needn't reach their ends.
Inputs may be any that keep to these rules, and one draw needn't show every extreme that they name: `expert_ids`: each row names 4 different experts; among the rows of one device no expert is named by more than 80 rows, and in some device some expert is named by exactly 80 rows. `priority`: each row orders the 128 tokens of one device, each number once. `cap_counts`: some expert has exactly 80.
All inputs are finite; a program needn't handle non-finite values. Where the reference program divides by a largest or mean magnitude, that divisor is 1e-20 or more.
Results may differ from the reference program's by a relative error of at most 0.017.
Values may be sent and summed in bfloat16 or wider, within the bound.
A program may use at most 128 MiB of HBM per device.

```python
import math
import jax
import jax.numpy as jnp
import numpy as np
from jax import lax

D = 1536
FH = 1536
TOP = 4
TOK_DEV = 128
EXPERTS = 8
TOKENS = 4096
CAP = 80
N_EP = 8
N_DP = 4


def draw_cap_counts(key, part):
    first_key, second_key = jax.random.split(jax.random.fold_in(key, 17))
    counts = jax.random.randint(first_key, (EXPERTS,), CAP // 2, CAP + 1)
    chosen = jax.random.randint(second_key, (), 0, EXPERTS)
    return jnp.where(jnp.arange(EXPERTS) == chosen, CAP, counts).astype(jnp.int32)


def level_of(own_key, dims, shards, smallest, largest):
    level, own = 1.0, jax.random.fold_in(own_key, 6)
    for dim, shards_of in shards:
        draws = jnp.exp(jax.random.uniform(jax.random.fold_in(own, dim), (shards_of,), jnp.float32, smallest / len(shards), largest / len(shards)))
        level = level * jnp.repeat(draws, dims[dim] // shards_of).reshape([-1 if axis == dim else 1 for axis in range(len(dims))])
    return level


def deal_out(rng, own, number, rows, amount, top, bound, slope):
    order = jax.random.permutation(rng, amount)
    crowded, common = load_shares(amount, rows * top, bound, slope, True), load_shares(amount, rows * top, bound, slope, False)
    places = jnp.arange(amount)

    def named(tallies, rotation):
        used = int((tallies > 0).sum())
        fixed = max(1, used // 4)
        passed = fixed + (places - fixed + rotation * (used - fixed)) % max(1, amount - fixed)
        return jnp.zeros((amount,), jnp.int32).at[order[jnp.where(places < fixed, places, passed)]].set(jnp.asarray(tallies, jnp.int32))

    tallies = jnp.where(number % 4 == 0, named(crowded, number // 4), named(common, number - number // 4 - 1))
    mixed = jax.random.permutation(jax.random.fold_in(own, 3), amount)
    source_of, sink = mixed[0:amount // 2 * 2:2], mixed[1:amount // 2 * 2:2]
    room = jnp.minimum(tallies[source_of] - 1, bound - tallies[sink]) // 2
    room = jnp.where((source_of == order[0]) | (sink == order[0]) | (tallies[sink] == 0), 0, jnp.maximum(room, 0))
    passed = jax.random.randint(jax.random.fold_in(own, 4), (amount // 2,), 0, 1 << 20) % (room + 1)
    tallies = tallies.at[source_of].add(-passed).at[sink].add(passed)
    members = jnp.searchsorted(jnp.cumsum(tallies), jnp.arange(rows * top), side="right").astype(jnp.int32)
    table = members.reshape(top, rows).T
    table = table[jax.random.permutation(jax.random.fold_in(own, 1), rows)]
    rotation = jax.random.randint(jax.random.fold_in(own, 2), (rows, 1), 0, top)
    return jnp.take_along_axis(table, (jnp.arange(top)[None, :] + rotation) % top, axis=1)


def load_shares(amount, total, bound, slope, full):
    loads = [(1 << 20) // math.isqrt(rank ** slope) + 1 for rank in range(1, amount + 1)]
    largest = bound if full else min(bound, max(-(-total // amount), total * loads[0] // sum(loads)))
    least = 1 if total - largest >= amount - 1 else 0
    given, surplus = [largest] + [least] * (amount - 1), total - largest - least * (amount - 1)
    while surplus > 0:
        candidates = [i for i in range(1, amount) if given[i] < largest] or [i for i in range(1, amount) if given[i] < bound]
        whole, budget = sum([loads[i] for i in candidates]), surplus
        for i in candidates:
            addition = min(bound - given[i], max(1, budget * loads[i] // whole), surplus)
            given[i] = given[i] + addition
            surplus = surplus - addition
    return np.array(given)


def gaussian(own_key, extent, scale, reach, cuts=(), kind=jnp.bfloat16):
    loudness = level_of(own_key, extent, cuts, -0.22, 0.18) if cuts else 1.0
    entries = jax.random.normal(own_key, extent, jnp.float32) * scale * loudness
    return jnp.minimum(jnp.maximum(entries, -reach), reach).astype(kind)


def setup_inputs(seed: int = 0) -> dict:
    key_of = jax.random.split(jax.random.key(seed), 10)
    grad_out = gaussian(key_of[0], (TOKENS, D), 1.0, 6.0, ((0, 32),), jnp.float32)
    tokens = gaussian(key_of[1], (TOKENS, D), 1.0, 6.0, ((0, 32),))
    probs = jnp.clip(0.1 + 0.4 * jax.random.uniform(key_of[2], (TOKENS, TOP), jnp.float32) ** level_of(key_of[2], (TOKENS, TOP), ((0, 32),), -0.2, 0.2), 0.1, 0.5)
    expert_ids_keys = jax.random.split(jax.random.fold_in(key_of[3], 1), TOKENS // TOK_DEV)
    expert_ids_turns = jax.random.permutation(jax.random.fold_in(key_of[3], 3), TOKENS // TOK_DEV)
    expert_ids = jax.vmap(lambda own, number: deal_out(jax.random.fold_in(key_of[3], 2), own, number, TOK_DEV, EXPERTS, TOP, CAP, 2))(expert_ids_keys, expert_ids_turns).reshape((TOKENS, TOP))
    priority = jax.vmap(lambda own: jax.random.permutation(own, TOK_DEV))(jax.random.split(key_of[4], (N_EP * N_DP))).reshape((N_EP * N_DP, TOK_DEV)).astype(jnp.int32)
    cap_counts = draw_cap_counts(jax.random.fold_in(key_of[9], 71), 0)
    gate_weight = gaussian(key_of[6], (EXPERTS, FH, D), D ** -0.5, 0.15625, ((0, 8),))
    up_weight = gaussian(key_of[7], (EXPERTS, FH, D), D ** -0.5, 0.15625, ((0, 8),))
    down_weight = gaussian(key_of[8], (EXPERTS, FH, D), D ** -0.5, 0.15625, ((0, 8),))
    return dict(grad_out=grad_out, tokens=tokens, probs=probs, expert_ids=expert_ids, priority=priority, cap_counts=cap_counts, gate_weight=gate_weight, up_weight=up_weight, down_weight=down_weight)


sharpness = 1.702


def contract_last(first_op, second_op):
    return lax.dot_general(first_op, second_op, (((1,), (1,)), ((), ())), preferred_element_type=jnp.float32)


def replica_sum(deltas, values):
    per_replica = N_EP * CAP
    partials = jnp.einsum("rsf,rsd->rfd", deltas.reshape(N_DP, per_replica, FH).astype(jnp.float32), values.reshape(N_DP, per_replica, D).astype(jnp.float32), precision=lax.Precision.HIGHEST)
    rounded = lax.optimization_barrier(partials.astype(jnp.bfloat16))
    return jnp.sum(rounded.astype(jnp.float32), axis=0).astype(jnp.bfloat16)


def reference(grad_out, tokens, probs, expert_ids, priority, cap_counts, gate_weight, up_weight, down_weight):
    blocks = N_EP * N_DP
    slot_rows = N_EP * CAP
    total_slots = N_DP * slot_rows
    block_ids = expert_ids.reshape(blocks, TOK_DEV, TOP)
    expert_range = jnp.arange(EXPERTS, dtype=jnp.int32)
    routed = jnp.any(block_ids[:, :, :, None] == expert_range, axis=2).astype(jnp.float32)
    earlier = (priority[:, None, :] < priority[:, :, None]).astype(jnp.float32)
    before = jnp.einsum("bsu,bue->bse", earlier, routed, precision=lax.Precision.HIGHEST)
    slot_rank = jnp.take_along_axis(before, block_ids, axis=2).astype(jnp.int32)
    kept = slot_rank < cap_counts[block_ids]
    block_range = jnp.arange(blocks, dtype=jnp.int32)
    source = block_range // N_DP
    replica = block_range % N_DP
    position = (replica[:, None, None] * slot_rows + source[:, None, None] * CAP + slot_rank).reshape(TOKENS, TOP)
    kept = kept.reshape(TOKENS, TOP)
    row_scale = jnp.maximum(jnp.max(jnp.abs(grad_out), axis=1), 1.0)
    quantized = (grad_out / row_scale[:, None]).astype(jnp.bfloat16)

    def one_expert(running, inputs):
        input_acc, prob_acc = running
        expert, w_gate, w_up, w_down = inputs
        live_pair = kept & (expert_ids == expert)
        target = jnp.where(live_pair, position, total_slots).astype(jnp.int32)
        input_buf = jnp.zeros((total_slots + 1, D), jnp.bfloat16)
        grad_buf = jnp.zeros((total_slots + 1, D), jnp.bfloat16)
        scale_buf = jnp.zeros((total_slots + 1,), jnp.float32)
        prob_buf = jnp.zeros((total_slots + 1,), jnp.float32)
        for which in range(TOP):
            input_buf = input_buf.at[target[:, which]].set(tokens)
            grad_buf = grad_buf.at[target[:, which]].set(quantized)
            scale_buf = scale_buf.at[target[:, which]].set(row_scale)
            prob_buf = prob_buf.at[target[:, which]].set(probs[:, which])
        slot_x = input_buf[:total_slots]
        slot_q = grad_buf[:total_slots]
        slot_scale = scale_buf[:total_slots]
        slot_prob = prob_buf[:total_slots]
        gate_pre = contract_last(slot_x, w_gate)
        up_pre = contract_last(slot_x, w_up)
        back_proj = contract_last(slot_q, w_down)
        squash = jax.nn.sigmoid(sharpness * gate_pre)
        gated = gate_pre * squash
        activated = (up_pre + 1.0) * gated
        weight = (slot_scale * slot_prob)[:, None]
        act_delta = weight * back_proj
        up_delta = (act_delta * gated).astype(jnp.bfloat16)
        gate_delta = (act_delta * (up_pre + 1.0) * (squash + sharpness * gate_pre * squash * (1.0 - squash))).astype(jnp.bfloat16)
        act_scaled = (activated * weight).astype(jnp.bfloat16)
        slot_in = (jnp.dot(gate_delta, w_gate, preferred_element_type=jnp.float32) + jnp.dot(up_delta, w_up, preferred_element_type=jnp.float32)).astype(jnp.bfloat16)
        slot_pgrad = slot_scale * jnp.sum(activated * back_proj, axis=1)
        pad_in = jnp.concatenate([slot_in, jnp.zeros((1, D), jnp.bfloat16)], axis=0)
        pad_prob = jnp.concatenate([slot_pgrad, jnp.zeros((1,), jnp.float32)], axis=0)
        for which in range(TOP):
            input_acc = input_acc + pad_in[target[:, which]].astype(jnp.float32)
        prob_acc = prob_acc + pad_prob[target]
        grads = (replica_sum(gate_delta, slot_x), replica_sum(up_delta, slot_x), replica_sum(act_scaled, slot_q))
        return (input_acc, prob_acc), grads

    start = (jnp.zeros((TOKENS, D), jnp.float32), jnp.zeros((TOKENS, TOP), jnp.float32))
    (input_acc, prob_acc), grads = lax.scan(one_expert, start, (expert_range, gate_weight, up_weight, down_weight))
    return input_acc.astype(jnp.bfloat16), prob_acc, grads[0], grads[1], grads[2]
```

```python
import functools

import jax
import jax.numpy as jnp
from jax import lax
from jax.experimental import pallas as pl
from jax.experimental.pallas import tpu as pltpu
from jax.sharding import PartitionSpec as P


sharpness = 1.702


def contract_last(first_op, second_op):
    return lax.dot_general(
        first_op, second_op, (((1,), (1,)), ((), ())), preferred_element_type=jnp.float32
    )


def contract_first(first_op, second_op):
    return lax.dot_general(
        first_op, second_op, (((0,), (0,)), ((), ())), preferred_element_type=jnp.float32
    )


def route_table(expert_ids, priority, cap_counts, buckets, capacity):
    ranking = priority[0]
    earlier = (ranking[None, :] < ranking[:, None]).astype(jnp.bfloat16)
    expert_range = lax.broadcasted_iota(jnp.int32, (1, 1, buckets), 2)
    matches = (expert_ids[:, :, None] == expert_range).astype(jnp.float32)
    routed = jnp.sum(matches, axis=1).astype(jnp.bfloat16)
    before = jnp.dot(earlier, routed, preferred_element_type=jnp.float32)
    slot_rank = jnp.sum(matches * before[:, None, :], axis=2).astype(jnp.int32)
    keep_limit = jnp.sum(matches * cap_counts.astype(jnp.float32)[None, None, :], axis=2)
    kept = slot_rank < keep_limit.astype(jnp.int32)
    return jnp.where(kept, expert_ids * capacity + slot_rank, -1)


def exchange_dispatch(tokens, quantized, pair_weight, placement, ep_size, capacity):
    table = jnp.any(placement, axis=1).astype(jnp.bfloat16)
    bucket_shape = (ep_size, capacity, tokens.shape[1])
    send_x = contract_first(table, tokens).astype(jnp.bfloat16)
    send_q = contract_first(table, quantized).astype(jnp.bfloat16)
    send_weight = jnp.sum(jnp.where(placement, pair_weight[:, :, None], 0.0), axis=(0, 1))
    slot_x = exchange(send_x.reshape(bucket_shape), "ep").reshape(-1, tokens.shape[1])
    slot_q = exchange(send_q.reshape(bucket_shape), "ep").reshape(-1, tokens.shape[1])
    weight = exchange(send_weight.reshape(ep_size, capacity), "ep").reshape(-1)
    return slot_x, slot_q, weight


def relay_dispatch(tokens, quantized, target, pair_weight, capacity):
    ep_size, levels = lax.axis_size("ep"), lax.axis_size("ep") // 2
    me = lax.axis_index("ep")
    z, x = me // 2, me % 2
    meta = jnp.concatenate([target.astype(jnp.float32).T, pair_weight.T], axis=0)
    table = exchange(jnp.broadcast_to(meta[None], (ep_size, *meta.shape)), "ep")
    top = target.shape[1]
    slots = lax.broadcasted_iota(jnp.int32, (1, capacity, 1), 1).astype(jnp.float32)

    def hop(array, step, sign):
        sources = [h for h in range(levels) if 0 <= h - sign * (step - 1) < levels and 0 <= h + sign < levels]
        return lax.ppermute(
            array, "ep", [(2 * h + j, 2 * (h + sign) + j) for h in sources for j in range(2)]
        )

    def hit(block, expert):
        rows = lax.dynamic_index_in_dim(table, block, 0, keepdims=False)[:top]
        base = (expert * capacity).astype(jnp.float32)
        return jnp.any(rows[:, None, :] == slots + base, axis=0).astype(jnp.bfloat16)

    second = jnp.where(z == 0, 1, z - 1)
    third = jnp.where(z < 2, z + 2, z - 2)
    fourth = jnp.where(z == 0, 3, jnp.where(z == 1, 2, jnp.where(z == 2, 3, 0)))
    order = (z, second, third, fourth)
    own_hits = [hit(2 * h + x, me) for h in order]
    cross_hits = [hit(2 * h + x, me ^ 1) for h in order]
    inner = (z == 1) | (z == 2)

    def pick(hits, rows):
        return jnp.dot(hits, rows, preferred_element_type=jnp.float32).astype(jnp.bfloat16)

    def spread(block):
        up_one, down_one = hop(block, 1, 1), hop(block, 1, -1)
        up_two, down_two = hop(up_one, 2, 1), hop(down_one, 2, -1)
        up_three, down_three = hop(up_two, 3, 1), hop(down_two, 3, -1)
        held = (
            block,
            jnp.where(z == 0, down_one, up_one),
            jnp.where(z < 2, down_two, up_two),
            jnp.where(inner, down_one, jnp.where(z == 0, down_three, up_three)),
        )
        out = jnp.zeros((ep_size * capacity, block.shape[1]), jnp.bfloat16)
        for i in range(4):
            crossed = lax.ppermute(
                pick(cross_hits[i], held[i]), "ep", [(d, d ^ 1) for d in range(ep_size)]
            )
            kept_here = pick(own_hits[i], held[i])
            base = 2 * order[i]
            out = lax.dynamic_update_slice_in_dim(out, kept_here, (base + x) * capacity, 0)
            out = lax.dynamic_update_slice_in_dim(out, crossed, (base + 1 - x) * capacity, 0)
        return out, (up_one, down_one)

    slot_x, arrived = spread(tokens)
    quantized, _ = lax.optimization_barrier((quantized, arrived))
    slot_q, _ = spread(quantized)
    targets = table[:, :top, None, :]
    base = (me * capacity).astype(jnp.float32)
    weight = jnp.sum(
        jnp.where(targets == slots[None] + base, table[:, top:, None, :], 0.0), axis=(1, 3)
    )
    return slot_x, slot_q, weight.reshape(-1)


def exchange(array, axis):
    return lax.all_to_all(array, axis, split_axis=0, concat_axis=0, tiled=True)


def pair_scatter(deltas, values, after=None):
    dp_size = lax.axis_size("dp")
    hidden = deltas.shape[1]
    if dp_size != 4:
        part = contract_first(deltas, values).astype(jnp.bfloat16)
        return lax.psum_scatter(part, "dp", scatter_dimension=0, tiled=True), part
    share = hidden // dp_size
    me = lax.axis_index("dp")
    near, far = me ^ 1, me ^ 2

    def quarter(which):
        columns = lax.dynamic_slice_in_dim(deltas, which * share, share, 1)
        return contract_first(columns, values)

    def swap(array, bit):
        return lax.ppermute(array, "dp", [(i, i ^ bit) for i in range(dp_size)])

    from_near_far = swap(quarter(near ^ 2).astype(jnp.bfloat16), 1)
    from_near_own = swap(quarter(near).astype(jnp.bfloat16), 1)
    passed = (quarter(far) + from_near_far.astype(jnp.float32)).astype(jnp.bfloat16)
    from_far = swap(passed, 2)
    if after is not None:
        from_far, _ = lax.optimization_barrier((from_far, after))
    own = quarter(me) + from_near_own.astype(jnp.float32)
    return (own + from_far.astype(jnp.float32)).astype(jnp.bfloat16), passed


def on_device_body(
    grad_out, tokens, probs, expert_ids, priority, cap_counts, gate_weight, up_weight, down_weight
):
    ep_size = lax.axis_size("ep")
    tok_rows, model_width = tokens.shape
    route_count = expert_ids.shape[1]
    capacity = 5 * route_count * tok_rows // (4 * ep_size)
    slot_rows = ep_size * capacity
    bucket_shape = (ep_size, capacity, model_width)
    target = route_table(expert_ids, priority, cap_counts, ep_size, capacity)
    slot_range = lax.broadcasted_iota(jnp.int32, (1, 1, slot_rows), 2)
    placement = target[:, :, None] == slot_range
    row_scale = jnp.maximum(jnp.max(jnp.abs(grad_out), axis=1), 1.0)
    quantized = (grad_out / row_scale[:, None]).astype(jnp.bfloat16)
    pair_weight = probs * row_scale[:, None]
    if ep_size == 8:
        slot_x, slot_q, weight = relay_dispatch(tokens, quantized, target, pair_weight, capacity)
    else:
        slot_x, slot_q, weight = exchange_dispatch(
            tokens, quantized, pair_weight, placement, ep_size, capacity
        )
    weight = weight[:, None]
    w_gate = gate_weight[0]
    w_up = up_weight[0]
    w_down = down_weight[0]

    gate_pre = contract_last(slot_x, w_gate)
    up_pre = contract_last(slot_x, w_up)
    squash = jax.nn.sigmoid(sharpness * gate_pre)
    gated = gate_pre * squash
    activated = (up_pre + 1.0) * gated
    act_scaled = (activated * weight).astype(jnp.bfloat16)
    down_share, passed = pair_scatter(act_scaled, slot_q)
    later_q, _ = lax.optimization_barrier((slot_q, passed))
    back_proj = contract_last(later_q, w_down)
    act_delta = weight * back_proj
    up_delta = (act_delta * gated).astype(jnp.bfloat16)
    gate_delta = (
        act_delta * (up_pre + 1.0) * (squash + sharpness * gate_pre * squash * (1.0 - squash))
    ).astype(jnp.bfloat16)
    slot_out = jnp.sum(activated * back_proj, axis=1)
    gate_share, _ = pair_scatter(gate_delta, slot_x)
    up_share, _ = pair_scatter(up_delta, slot_x, gate_share)
    in_delta = jnp.dot(gate_delta, w_gate, preferred_element_type=jnp.float32) + jnp.dot(
        up_delta, w_up, preferred_element_type=jnp.float32
    )
    slot_in = in_delta.astype(jnp.bfloat16)
    back_in = exchange(slot_in.reshape(bucket_shape), "ep").reshape(slot_rows, model_width)
    back_prob = exchange(slot_out.reshape(ep_size, capacity), "ep").reshape(slot_rows)
    prob_grad = row_scale[:, None] * jnp.sum(
        jnp.where(placement, back_prob[None, None, :], 0.0), axis=2
    )
    table_low = jnp.any(placement, axis=1).astype(jnp.bfloat16)
    input_grad = jnp.dot(table_low, back_in, preferred_element_type=jnp.float32).astype(
        jnp.bfloat16
    )
    return (input_grad, prob_grad, gate_share[None], up_share[None], down_share[None])


MESH = pl.DeviceIdType.MESH


def fused_kernel(
    ep_size, dp_size, capacity, chunk,
    tokens_ref, grad_ref, probs_ref, ids_ref, prio_ref, caps_ref, gate_hbm, up_hbm, down_hbm,
    input_ref, prob_ref, grads_ref,
    w_gate, w_up, w_down, raw, slots, cross, deltas, gated_part, slope_part, act_part, weight_col,
    slot_sum, meta, target_col, scale_col, near_out, far_in, near_in, keep_out, keep_in, result,
    back, prob_out, prob_in,
    load_sem, own_send, relay_send, raw_recv, cross_send, cross_recv, meta_send, meta_recv,
    pass_send, pass_recv, keep_send, keep_recv, far_send, far_recv,
    ret_send, ret_recv, prob_send, prob_recv,
):
    tok_rows, width = tokens_ref.shape
    top = ids_ref.shape[1]
    hidden = w_gate.shape[0]
    share = hidden // dp_size
    chunks = width // chunk
    parts = hidden // chunk
    levels = ep_size // 2
    group = 2 * capacity
    units = 3 * chunks
    me, rep = lax.axis_index("ep"), lax.axis_index("dp")
    z, x = lax.div(me, 2), lax.rem(me, 2)
    partner = me + 1 - 2 * x
    near = rep + 1 - 2 * lax.rem(rep, 2)
    far = lax.rem(rep + 2, dp_size)
    diagonal = lax.rem(near + 2, dp_size)
    high = lax.div(z, 2)
    middle = lax.div(z * (levels - 1 - z), 2)
    end = (levels - 1) * high
    first_target = middle * end + (1 - middle) * (1 + high)
    second_target = 2 - high

    def level_at(place):
        last = lax.div(place, 3)
        inner = lax.rem(place + 1, 3) * (1 - last) + 3 * last
        low = (1 - middle) * place + middle * inner
        return (1 - high) * low + high * (levels - 1 - low)

    def cols(index, size=chunk):
        return pl.ds(pl.multiple_of(index * size, size), size)

    def rows(index, size):
        return pl.ds(pl.multiple_of(index * size, size), size)

    def raw_copy(tensor, level, index, target, sem):
        return pltpu.make_async_remote_copy(
            src_ref=raw.at[tensor, level, index],
            dst_ref=raw.at[tensor, level, index],
            send_sem=sem,
            recv_sem=raw_recv.at[tensor, level, index],
            device_id={"ep": 2 * target + x},
            device_id_type=MESH,
        )

    def own_copy(tensor, which, index):
        target = first_target if which == 0 else second_target
        return raw_copy(tensor, z, index, target, own_send.at[tensor, which, index])

    def relay_copy(tensor, place, index):
        sem = relay_send.at[tensor, lax.div(place, 2), index]
        return raw_copy(tensor, level_at(place), index, end, sem)

    def cross_copy(tensor, level, index):
        return pltpu.make_async_remote_copy(
            src_ref=cross.at[tensor, level, index],
            dst_ref=slots.at[tensor, rows(2 * level + x, capacity), cols(index)],
            send_sem=cross_send.at[tensor, level, index],
            recv_sem=cross_recv.at[tensor, level, index],
            device_id={"ep": partner},
            device_id_type=MESH,
        )

    def meta_copy(step):
        return pltpu.make_async_remote_copy(
            src_ref=meta.at[me],
            dst_ref=meta.at[me],
            send_sem=meta_send.at[step],
            recv_sem=meta_recv.at[me],
            device_id={"ep": lax.rem(me + step, ep_size)},
            device_id_type=MESH,
        )

    def meta_arrival(step):
        source = lax.rem(me + step, ep_size)
        return pltpu.make_async_remote_copy(
            src_ref=meta.at[source],
            dst_ref=meta.at[source],
            send_sem=meta_send.at[step],
            recv_sem=meta_recv.at[source],
            device_id={"ep": source},
            device_id_type=MESH,
        )

    def dp_copy(source, target, send, recv, peer):
        return pltpu.make_async_remote_copy(
            src_ref=source, dst_ref=target, send_sem=send, recv_sem=recv,
            device_id={"dp": peer}, device_id_type=MESH,
        )

    def pass_copy(unit):
        return dp_copy(
            near_out.at[lax.rem(unit, 2)], near_in.at[unit], pass_send.at[unit], pass_recv.at[unit], near
        )

    def keep_copy(unit):
        return dp_copy(
            keep_out.at[lax.rem(unit, 2)], keep_in.at[unit], keep_send.at[unit], keep_recv.at[unit], near
        )

    def far_copy(unit):
        return dp_copy(near_in.at[unit], far_in.at[unit], far_send.at[unit], far_recv.at[unit], far)

    def return_copy(block):
        return pltpu.make_async_remote_copy(
            src_ref=result.at[rows(block, capacity)],
            dst_ref=back.at[rows(me, capacity)],
            send_sem=ret_send.at[block],
            recv_sem=ret_recv.at[me],
            device_id={"ep": block},
            device_id_type=MESH,
        )

    def prob_copy(block):
        return pltpu.make_async_remote_copy(
            src_ref=prob_out.at[block],
            dst_ref=prob_in.at[me],
            send_sem=prob_send.at[block],
            recv_sem=prob_recv.at[me],
            device_id={"ep": block},
            device_id_type=MESH,
        )

    def return_arrival(source):
        return pltpu.make_async_remote_copy(
            src_ref=result.at[rows(source, capacity)],
            dst_ref=back.at[rows(source, capacity)],
            send_sem=ret_send.at[source],
            recv_sem=ret_recv.at[source],
            device_id={"ep": source},
            device_id_type=MESH,
        )

    def prob_arrival(source):
        return pltpu.make_async_remote_copy(
            src_ref=prob_out.at[source],
            dst_ref=prob_in.at[source],
            send_sem=prob_send.at[source],
            recv_sem=prob_recv.at[source],
            device_id={"ep": source},
            device_id_type=MESH,
        )

    loads = [
        pltpu.make_async_copy(source.at[0], target, load_sem.at[i])
        for i, (source, target) in enumerate(((gate_hbm, w_gate), (up_hbm, w_up), (down_hbm, w_down)))
    ]
    for load in loads:
        load.start()
    for index in range(chunks):
        raw[0, z, index] = tokens_ref[:, index * chunk : (index + 1) * chunk]

    barrier = pltpu.get_barrier_semaphore()
    for step in range(1, ep_size):
        pl.semaphore_signal(
            barrier, inc=1, device_id={"ep": lax.rem(me + step, ep_size)}, device_id_type=MESH
        )
    for peer in (near, far):
        pl.semaphore_signal(barrier, inc=1, device_id={"dp": peer}, device_id_type=MESH)
    pl.semaphore_wait(barrier, ep_size + 1)

    for index in range(chunks):
        own_copy(0, 0, index).start()
    scale = jnp.maximum(jnp.max(jnp.abs(grad_ref[...]), axis=1, keepdims=True), 1.0)
    scale_col[...] = scale
    for index in range(chunks):
        piece = grad_ref[:, index * chunk : (index + 1) * chunk]
        raw[1, z, index] = (piece / scale).astype(jnp.bfloat16)
    for index in range(chunks):
        own_copy(1, 0, index).start()
    for tensor in range(2):
        for index in range(chunks):
            own_copy(tensor, 1, index).start()

    square = (tok_rows, tok_rows)
    eye = lax.broadcasted_iota(jnp.int32, square, 0) == lax.broadcasted_iota(jnp.int32, square, 1)
    prio_row = prio_ref[...].astype(jnp.float32)
    prio_col = jnp.sum(jnp.where(eye, prio_row, 0.0), axis=1, keepdims=True)
    earlier = jnp.where(prio_row < prio_col, 1.0, 0.0).astype(jnp.bfloat16)
    lane = lax.broadcasted_iota(jnp.int32, square, 1)
    caps = jnp.zeros((1, tok_rows), jnp.float32)
    for expert in range(ep_size):
        count = caps_ref[expert].astype(jnp.float32)
        caps = caps + jnp.where(lane[:1] == expert, count, 0.0)
    ids = ids_ref[...]
    matches = [jnp.where(ids[:, k : k + 1] == lane, 1.0, 0.0) for k in range(top)]
    routed = sum(matches[1:], matches[0]).astype(jnp.bfloat16)
    before = jnp.dot(earlier, routed, preferred_element_type=jnp.float32)
    pair_weight = probs_ref[...] * scale
    for k in range(top):
        rank = jnp.sum(matches[k] * before, axis=1, keepdims=True)
        limit = jnp.sum(matches[k] * caps, axis=1, keepdims=True)
        place = ids[:, k : k + 1].astype(jnp.float32) * capacity + rank
        target = jnp.where(rank < limit, place, -1.0)
        target_col[k] = target
        meta[me, k : k + 1, :] = jnp.sum(jnp.where(eye, target, 0.0), axis=0, keepdims=True)
        meta[me, top + k : top + k + 1, :] = jnp.sum(
            jnp.where(eye, pair_weight[:, k : k + 1], 0.0), axis=0, keepdims=True
        )
    for step in range(1, ep_size):
        meta_copy(step).start()
    for load in loads:
        load.wait()
    for step in range(1, ep_size):
        meta_arrival(step).wait_recv()

    slot_iota = lax.broadcasted_iota(jnp.int32, (capacity, tok_rows), 0)

    def slot_names(expert):
        return (slot_iota + expert * capacity).astype(jnp.float32)

    def hits(level, expert):
        table, names = meta[2 * level + x], slot_names(expert)
        total = jnp.zeros((capacity, tok_rows), jnp.float32)
        for k in range(top):
            total = total + jnp.where(table[k : k + 1] == names, 1.0, 0.0)
        return total.astype(jnp.bfloat16)

    def event(tensor, place, index):
        level = level_at(place)

        @pl.when(place > 0)
        def _():
            raw_copy(tensor, level, index, end, relay_send.at[tensor, 0, index]).wait_recv()

        @pl.when(middle * lax.rem(place, 2) == 1)
        def _():
            relay_copy(tensor, place, index).start()

        block = raw[tensor, level, index]
        crossed = jnp.dot(hits(level, partner), block, preferred_element_type=jnp.float32)
        cross[tensor, level, index] = crossed.astype(jnp.bfloat16)
        cross_copy(tensor, level, index).start()
        kept = jnp.dot(hits(level, me), block, preferred_element_type=jnp.float32)
        slots[tensor, rows(2 * level + x, capacity), cols(index)] = kept.astype(jnp.bfloat16)

    def forward_part(place, part):
        level = level_at(place)

        @pl.when(part == 0)
        def _():
            for index in range(chunks):
                cross_copy(0, level, index).wait_recv()
            names = slot_names(me)
            for column in range(2):
                table = meta[2 * level + column]
                total = jnp.zeros((capacity, tok_rows), jnp.float32)
                for k in range(top):
                    total = total + jnp.where(
                        table[k : k + 1] == names, table[top + k : top + k + 1], 0.0
                    )
                weight_col[column * capacity : (column + 1) * capacity, :] = jnp.sum(
                    total, axis=1, keepdims=True
                )

        entries = slots[0, rows(level, group), :]
        gate_pre = contract_last(entries, w_gate[rows(part, chunk), :])
        up_one = contract_last(entries, w_up[rows(part, chunk), :]) + 1.0
        squash = jax.nn.sigmoid(sharpness * gate_pre)
        gated = gate_pre * squash
        activated = up_one * gated
        gated_part[part] = gated
        slope_part[part] = up_one * (squash + sharpness * gated * (1.0 - squash))
        act_part[part] = activated
        deltas[0, rows(level, group), cols(part)] = (activated * weight_col[...]).astype(jnp.bfloat16)

    def backward_part(place, part, wait):
        level = level_at(place)
        if wait:

            @pl.when(part == 0)
            def _():
                for index in range(chunks):
                    cross_copy(1, level, index).wait_recv()

        entries = slots[1, rows(level, group), :]
        back_proj = contract_last(entries, w_down[rows(part, chunk), :])
        act_delta = weight_col[...] * back_proj
        deltas[1, rows(level, group), cols(part)] = (act_delta * slope_part[part]).astype(jnp.bfloat16)
        deltas[2, rows(level, group), cols(part)] = (act_delta * gated_part[part]).astype(jnp.bfloat16)
        slot_sum[part] = jnp.sum(act_part[part] * back_proj, axis=1, keepdims=True)

        @pl.when(part == parts - 1)
        def _():
            total = slot_sum[0]
            for other in range(1, parts):
                total = total + slot_sum[other]
            cap_square = (capacity, tok_rows)
            diagonal_mask = lax.broadcasted_iota(jnp.int32, cap_square, 1) == slot_iota
            for column in range(2):
                line = total[column * capacity : (column + 1) * capacity]
                line = jnp.sum(jnp.where(diagonal_mask, line, 0.0), axis=0, keepdims=True)
                prob_out[2 * level + column] = jnp.broadcast_to(line, prob_out.shape[1:])

    def exchange_step(place, carry):
        def token_step(index, inner):
            event(0, place, index)

            @pl.when(place > 0)
            def _():
                backward_part(place - 1, index, True)

            return inner

        def grad_step(index, inner):
            event(1, place, index)
            forward_part(place, index)
            return inner

        lax.fori_loop(0, chunks, token_step, 0)
        lax.fori_loop(0, chunks, grad_step, 0)
        return carry

    lax.fori_loop(0, levels, exchange_step, 0)

    def send_back():
        def level_step(level, carry):
            def column_step(index, inner):
                total = jnp.dot(
                    deltas[1, rows(level, group), :], w_gate[:, cols(index)],
                    preferred_element_type=jnp.float32,
                ) + jnp.dot(
                    deltas[2, rows(level, group), :], w_up[:, cols(index)],
                    preferred_element_type=jnp.float32,
                )
                result[rows(level, group), cols(index)] = total.astype(jnp.bfloat16)
                return inner

            lax.fori_loop(0, chunks, column_step, 0)
            for column in range(2):
                block = 2 * level + column

                @pl.when(block != me)
                def _():
                    return_copy(block).start()
                    prob_copy(block).start()

                @pl.when(block == me)
                def _():
                    back[rows(me, capacity), :] = result[rows(me, capacity), :]
                    prob_in[me] = prob_out[me]

            return carry

        lax.fori_loop(0, levels, level_step, 0)

    def partial_of(unit, quarter):
        tensor, index = lax.div(unit, chunks), lax.rem(unit, chunks)
        values = slots[1 - lax.div(tensor + 1, 2), :, cols(index)]
        return contract_first(deltas[tensor, :, cols(quarter, share)], values)

    def reduce_step(unit, carry):
        @pl.when(unit < chunks)
        def _():
            cross_copy(1, level_at(levels - 1), lax.rem(unit, chunks)).wait_recv()

        @pl.when(unit == chunks)
        def _():
            def last_step(part, inner):
                backward_part(levels - 1, part, False)
                return inner

            lax.fori_loop(0, parts, last_step, 0)

        @pl.when(unit == chunks + 1)
        def _():
            send_back()

        slot = lax.rem(unit, 2)

        @pl.when(unit >= 2)
        def _():
            pass_copy(unit - 2).wait_send()
            keep_copy(unit - 2).wait_send()

        near_out[slot] = partial_of(unit, diagonal).astype(jnp.bfloat16)
        pass_copy(unit).start()
        passed = partial_of(unit, far)
        pass_copy(unit).wait_recv()
        near_in[unit] = (passed + near_in[unit].astype(jnp.float32)).astype(jnp.bfloat16)
        far_copy(unit).start()
        keep_out[slot] = partial_of(unit, near).astype(jnp.bfloat16)
        keep_copy(unit).start()
        return carry

    lax.fori_loop(0, units, reduce_step, 0)

    def combine():
        for step in range(1, ep_size):
            source = lax.rem(me + step, ep_size)
            return_arrival(source).wait_recv()
            prob_arrival(source).wait_recv()
        shape = (tok_rows, ep_size * capacity)
        names = lax.broadcasted_iota(jnp.int32, shape, 1).astype(jnp.float32)
        table = jnp.zeros(shape, jnp.float32)
        for k in range(top):
            table = table + jnp.where(target_col[k] == names, 1.0, 0.0)
        table = table.astype(jnp.bfloat16)
        for index in range(chunks):
            span = slice(index * chunk, (index + 1) * chunk)
            input_ref[:, span] = jnp.dot(
                table, back[:, span], preferred_element_type=jnp.float32
            ).astype(jnp.bfloat16)
        lane_name = lane.astype(jnp.float32)
        for k in range(top):
            total = jnp.zeros((tok_rows, tok_rows), jnp.float32)
            for expert in range(ep_size):
                found = target_col[k] == lane_name + float(expert * capacity)
                total = total + jnp.where(found, prob_in[expert][:1], 0.0)
            prob_ref[:, k : k + 1] = scale_col[...] * jnp.sum(total, axis=1, keepdims=True)

    def finish_step(unit, carry):
        @pl.when(unit == units - 2)
        def _():
            combine()

        total = partial_of(unit, rep)
        keep_copy(unit).wait_recv()
        total = total + keep_in[unit].astype(jnp.float32)
        far_copy(unit).wait_recv()
        tensor, index = lax.div(unit, chunks), lax.rem(unit, chunks)
        grads_ref[tensor, :, cols(index)] = (total + far_in[unit].astype(jnp.float32)).astype(
            jnp.bfloat16
        )
        return carry

    lax.fori_loop(0, units, finish_step, 0)

    for tensor in range(2):
        for index in range(chunks):
            own_copy(tensor, 0, index).wait_send()
            own_copy(tensor, 1, index).wait_send()

            @pl.when(middle == 1)
            def _():
                relay_copy(tensor, 1, index).wait_send()
                relay_copy(tensor, 3, index).wait_send()

            for level in range(levels):
                cross_copy(tensor, level, index).wait_send()
    for step in range(1, ep_size):
        meta_copy(step).wait_send()
        peer = lax.rem(me + step, ep_size)
        return_copy(peer).wait_send()
        prob_copy(peer).wait_send()
    for unit in (units - 2, units - 1):
        pass_copy(unit).wait_send()
        keep_copy(unit).wait_send()
    for unit in range(units):
        far_copy(unit).wait_send()


def fused_body(
    grad_out, tokens, probs, expert_ids, priority, cap_counts, gate_weight, up_weight, down_weight
):
    ep_size, dp_size = lax.axis_size("ep"), lax.axis_size("dp")
    tok_rows, width = tokens.shape
    top = expert_ids.shape[1]
    hidden = gate_weight.shape[1]
    capacity = 5 * top * tok_rows // (4 * ep_size)
    slot_rows = ep_size * capacity
    chunk = width // 3
    chunks, parts, levels = width // chunk, hidden // chunk, ep_size // 2
    share = hidden // dp_size
    units = 3 * chunks
    bf16, f32 = jnp.bfloat16, jnp.float32
    vmem, dma = pltpu.VMEM, pltpu.SemaphoreType.DMA
    in_vmem = pl.BlockSpec(memory_space=pltpu.VMEM)
    anywhere = pl.BlockSpec(memory_space=pl.ANY)
    scratch = [
        vmem((hidden, width), bf16), vmem((hidden, width), bf16), vmem((hidden, width), bf16),
        vmem((2, levels, chunks, tok_rows, chunk), bf16),
        vmem((2, slot_rows, width), bf16),
        vmem((2, levels, chunks, capacity, chunk), bf16),
        vmem((3, slot_rows, hidden), bf16),
        vmem((parts, 2 * capacity, chunk), f32),
        vmem((parts, 2 * capacity, chunk), f32),
        vmem((parts, 2 * capacity, chunk), f32),
        vmem((2 * capacity, 1), f32),
        vmem((parts, 2 * capacity, 1), f32),
        vmem((ep_size, 2 * top, tok_rows), f32),
        vmem((top, tok_rows, 1), f32),
        vmem((tok_rows, 1), f32),
        vmem((2, share, chunk), bf16),
        vmem((units, share, chunk), bf16),
        vmem((units, share, chunk), bf16),
        vmem((2, share, chunk), bf16),
        vmem((units, share, chunk), bf16),
        vmem((slot_rows, width), bf16),
        vmem((slot_rows, width), bf16),
        vmem((ep_size, 8, tok_rows), f32),
        vmem((ep_size, 8, tok_rows), f32),
        dma((3,)), dma((2, 2, chunks)), dma((2, 2, chunks)), dma((2, levels, chunks)),
        dma((2, levels, chunks)), dma((2, levels, chunks)), dma((ep_size,)), dma((ep_size,)),
        dma((units,)), dma((units,)), dma((units,)), dma((units,)), dma((units,)), dma((units,)),
        dma((ep_size,)), dma((ep_size,)), dma((ep_size,)), dma((ep_size,)),
    ]
    input_grad, prob_grad, grads = pl.pallas_call(
        functools.partial(fused_kernel, ep_size, dp_size, capacity, chunk),
        out_shape=(
            jax.ShapeDtypeStruct((tok_rows, width), bf16),
            jax.ShapeDtypeStruct((tok_rows, top), f32),
            jax.ShapeDtypeStruct((3, share, width), bf16),
        ),
        in_specs=[in_vmem] * 5 + [pl.BlockSpec(memory_space=pltpu.SMEM)] + [anywhere] * 3,
        out_specs=(in_vmem, in_vmem, in_vmem),
        scratch_shapes=scratch,
        compiler_params=pltpu.CompilerParams(
            collective_id=0, has_side_effects=True, vmem_limit_bytes=66_000_000
        ),
        name="fused_step",
    )(tokens, grad_out, probs, expert_ids, priority, cap_counts, gate_weight, up_weight, down_weight)
    return input_grad, prob_grad, grads[1][None], grads[2][None], grads[0][None]


def on_device(*arrays):
    return on_device_body(*arrays)


def solution(mesh):
    fused = mesh.shape["ep"] == 8 and mesh.shape["dp"] == 4
    return jax.shard_map(
        fused_body if fused else on_device,
        mesh=mesh,
        in_specs=(
            P(("ep", "dp"), None),
            P(("ep", "dp"), None),
            P(("ep", "dp"), None),
            P(("ep", "dp"), None),
            P(("ep", "dp"), None),
            P(),
            P("ep", None, None),
            P("ep", None, None),
            P("ep", None, None),
        ),
        out_specs=(
            P(("ep", "dp"), None),
            P(("ep", "dp"), None),
            P("ep", "dp", None),
            P("ep", "dp", None),
            P("ep", "dp", None),
        ),
        check_vma=False,
    )
```

```python
import functools

import jax
import jax.numpy as jnp
from jax import lax
from jax.experimental import pallas as pl
from jax.experimental.pallas import tpu as pltpu
from jax.sharding import PartitionSpec as P


sharpness = 1.702


def contract_last(first_op, second_op):
    return lax.dot_general(
        first_op, second_op, (((1,), (1,)), ((), ())), preferred_element_type=jnp.float32
    )


def contract_first(first_op, second_op):
    return lax.dot_general(
        first_op, second_op, (((0,), (0,)), ((), ())), preferred_element_type=jnp.float32
    )


def route_table(expert_ids, priority, cap_counts, buckets, capacity):
    ranking = priority[0]
    earlier = (ranking[None, :] < ranking[:, None]).astype(jnp.bfloat16)
    expert_range = lax.broadcasted_iota(jnp.int32, (1, 1, buckets), 2)
    matches = (expert_ids[:, :, None] == expert_range).astype(jnp.float32)
    routed = jnp.sum(matches, axis=1).astype(jnp.bfloat16)
    before = jnp.dot(earlier, routed, preferred_element_type=jnp.float32)
    slot_rank = jnp.sum(matches * before[:, None, :], axis=2).astype(jnp.int32)
    keep_limit = jnp.sum(matches * cap_counts.astype(jnp.float32)[None, None, :], axis=2)
    kept = slot_rank < keep_limit.astype(jnp.int32)
    return jnp.where(kept, expert_ids * capacity + slot_rank, -1)


def exchange_dispatch(tokens, quantized, pair_weight, placement, ep_size, capacity):
    table = jnp.any(placement, axis=1).astype(jnp.bfloat16)
    bucket_shape = (ep_size, capacity, tokens.shape[1])
    send_x = contract_first(table, tokens).astype(jnp.bfloat16)
    send_q = contract_first(table, quantized).astype(jnp.bfloat16)
    send_weight = jnp.sum(jnp.where(placement, pair_weight[:, :, None], 0.0), axis=(0, 1))
    slot_x = exchange(send_x.reshape(bucket_shape), "ep").reshape(-1, tokens.shape[1])
    slot_q = exchange(send_q.reshape(bucket_shape), "ep").reshape(-1, tokens.shape[1])
    weight = exchange(send_weight.reshape(ep_size, capacity), "ep").reshape(-1)
    return slot_x, slot_q, weight


def relay_dispatch(tokens, quantized, target, pair_weight, capacity):
    ep_size, levels = lax.axis_size("ep"), lax.axis_size("ep") // 2
    me = lax.axis_index("ep")
    z, x = me // 2, me % 2
    meta = jnp.concatenate([target.astype(jnp.float32).T, pair_weight.T], axis=0)
    table = exchange(jnp.broadcast_to(meta[None], (ep_size, *meta.shape)), "ep")
    top = target.shape[1]
    slots = lax.broadcasted_iota(jnp.int32, (1, capacity, 1), 1).astype(jnp.float32)

    def hop(array, step, sign):
        sources = [h for h in range(levels) if 0 <= h - sign * (step - 1) < levels and 0 <= h + sign < levels]
        return lax.ppermute(
            array, "ep", [(2 * h + j, 2 * (h + sign) + j) for h in sources for j in range(2)]
        )

    def hit(block, expert):
        rows = lax.dynamic_index_in_dim(table, block, 0, keepdims=False)[:top]
        base = (expert * capacity).astype(jnp.float32)
        return jnp.any(rows[:, None, :] == slots + base, axis=0).astype(jnp.bfloat16)

    second = jnp.where(z == 0, 1, z - 1)
    third = jnp.where(z < 2, z + 2, z - 2)
    fourth = jnp.where(z == 0, 3, jnp.where(z == 1, 2, jnp.where(z == 2, 3, 0)))
    order = (z, second, third, fourth)
    own_hits = [hit(2 * h + x, me) for h in order]
    cross_hits = [hit(2 * h + x, me ^ 1) for h in order]
    inner = (z == 1) | (z == 2)

    def pick(hits, rows):
        return jnp.dot(hits, rows, preferred_element_type=jnp.float32).astype(jnp.bfloat16)

    def spread(block):
        up_one, down_one = hop(block, 1, 1), hop(block, 1, -1)
        up_two, down_two = hop(up_one, 2, 1), hop(down_one, 2, -1)
        up_three, down_three = hop(up_two, 3, 1), hop(down_two, 3, -1)
        held = (
            block,
            jnp.where(z == 0, down_one, up_one),
            jnp.where(z < 2, down_two, up_two),
            jnp.where(inner, down_one, jnp.where(z == 0, down_three, up_three)),
        )
        out = jnp.zeros((ep_size * capacity, block.shape[1]), jnp.bfloat16)
        for i in range(4):
            crossed = lax.ppermute(
                pick(cross_hits[i], held[i]), "ep", [(d, d ^ 1) for d in range(ep_size)]
            )
            kept_here = pick(own_hits[i], held[i])
            base = 2 * order[i]
            out = lax.dynamic_update_slice_in_dim(out, kept_here, (base + x) * capacity, 0)
            out = lax.dynamic_update_slice_in_dim(out, crossed, (base + 1 - x) * capacity, 0)
        return out, (up_one, down_one)

    slot_x, arrived = spread(tokens)
    quantized, _ = lax.optimization_barrier((quantized, arrived))
    slot_q, _ = spread(quantized)
    targets = table[:, :top, None, :]
    base = (me * capacity).astype(jnp.float32)
    weight = jnp.sum(
        jnp.where(targets == slots[None] + base, table[:, top:, None, :], 0.0), axis=(1, 3)
    )
    return slot_x, slot_q, weight.reshape(-1)


def exchange(array, axis):
    return lax.all_to_all(array, axis, split_axis=0, concat_axis=0, tiled=True)


def pair_scatter(deltas, values, after=None):
    dp_size = lax.axis_size("dp")
    hidden = deltas.shape[1]
    if dp_size != 4:
        part = contract_first(deltas, values).astype(jnp.bfloat16)
        return lax.psum_scatter(part, "dp", scatter_dimension=0, tiled=True), part
    share = hidden // dp_size
    me = lax.axis_index("dp")
    near, far = me ^ 1, me ^ 2

    def quarter(which):
        columns = lax.dynamic_slice_in_dim(deltas, which * share, share, 1)
        return contract_first(columns, values)

    def swap(array, bit):
        return lax.ppermute(array, "dp", [(i, i ^ bit) for i in range(dp_size)])

    from_near_far = swap(quarter(near ^ 2).astype(jnp.bfloat16), 1)
    from_near_own = swap(quarter(near).astype(jnp.bfloat16), 1)
    passed = (quarter(far) + from_near_far.astype(jnp.float32)).astype(jnp.bfloat16)
    from_far = swap(passed, 2)
    if after is not None:
        from_far, _ = lax.optimization_barrier((from_far, after))
    own = quarter(me) + from_near_own.astype(jnp.float32)
    return (own + from_far.astype(jnp.float32)).astype(jnp.bfloat16), passed


def on_device_body(
    grad_out, tokens, probs, expert_ids, priority, cap_counts, gate_weight, up_weight, down_weight
):
    ep_size = lax.axis_size("ep")
    tok_rows, model_width = tokens.shape
    route_count = expert_ids.shape[1]
    capacity = 5 * route_count * tok_rows // (4 * ep_size)
    slot_rows = ep_size * capacity
    bucket_shape = (ep_size, capacity, model_width)
    target = route_table(expert_ids, priority, cap_counts, ep_size, capacity)
    slot_range = lax.broadcasted_iota(jnp.int32, (1, 1, slot_rows), 2)
    placement = target[:, :, None] == slot_range
    row_scale = jnp.maximum(jnp.max(jnp.abs(grad_out), axis=1), 1.0)
    quantized = (grad_out / row_scale[:, None]).astype(jnp.bfloat16)
    pair_weight = probs * row_scale[:, None]
    if ep_size == 8:
        slot_x, slot_q, weight = relay_dispatch(tokens, quantized, target, pair_weight, capacity)
    else:
        slot_x, slot_q, weight = exchange_dispatch(
            tokens, quantized, pair_weight, placement, ep_size, capacity
        )
    weight = weight[:, None]
    w_gate = gate_weight[0]
    w_up = up_weight[0]
    w_down = down_weight[0]

    gate_pre = contract_last(slot_x, w_gate)
    up_pre = contract_last(slot_x, w_up)
    squash = jax.nn.sigmoid(sharpness * gate_pre)
    gated = gate_pre * squash
    activated = (up_pre + 1.0) * gated
    act_scaled = (activated * weight).astype(jnp.bfloat16)
    down_share, passed = pair_scatter(act_scaled, slot_q)
    later_q, _ = lax.optimization_barrier((slot_q, passed))
    back_proj = contract_last(later_q, w_down)
    act_delta = weight * back_proj
    up_delta = (act_delta * gated).astype(jnp.bfloat16)
    gate_delta = (
        act_delta * (up_pre + 1.0) * (squash + sharpness * gate_pre * squash * (1.0 - squash))
    ).astype(jnp.bfloat16)
    slot_out = jnp.sum(activated * back_proj, axis=1)
    gate_share, _ = pair_scatter(gate_delta, slot_x)
    up_share, _ = pair_scatter(up_delta, slot_x, gate_share)
    in_delta = jnp.dot(gate_delta, w_gate, preferred_element_type=jnp.float32) + jnp.dot(
        up_delta, w_up, preferred_element_type=jnp.float32
    )
    slot_in = in_delta.astype(jnp.bfloat16)
    back_in = exchange(slot_in.reshape(bucket_shape), "ep").reshape(slot_rows, model_width)
    back_prob = exchange(slot_out.reshape(ep_size, capacity), "ep").reshape(slot_rows)
    prob_grad = row_scale[:, None] * jnp.sum(
        jnp.where(placement, back_prob[None, None, :], 0.0), axis=2
    )
    table_low = jnp.any(placement, axis=1).astype(jnp.bfloat16)
    input_grad = jnp.dot(table_low, back_in, preferred_element_type=jnp.float32).astype(
        jnp.bfloat16
    )
    return (input_grad, prob_grad, gate_share[None], up_share[None], down_share[None])


MESH = pl.DeviceIdType.MESH


def fused_kernel(
    ep_size, dp_size, capacity, chunk,
    tokens_ref, grad_ref, probs_ref, ids_ref, prio_ref, caps_ref, gate_hbm, up_hbm, down_hbm,
    input_ref, prob_ref, grads_ref,
    w_gate, w_up, w_down, raw, slots, cross, deltas, gated_part, slope_part, act_part, weight_col,
    slot_sum, meta, target_col, scale_col, near_out, far_in, near_in, keep_out, keep_in, result,
    back, prob_out, prob_in,
    load_sem, own_send, relay_send, raw_recv, cross_send, cross_recv, meta_send, meta_recv,
    pass_send, pass_recv, keep_send, keep_recv, far_send, far_recv,
    ret_send, ret_recv, prob_send, prob_recv,
):
    tok_rows, width = tokens_ref.shape
    top = ids_ref.shape[0]
    hidden = w_gate.shape[0]
    share = hidden // dp_size
    chunks = width // chunk
    parts = hidden // chunk
    levels = ep_size // 2
    group = 2 * capacity
    units = 3 * chunks
    me, rep = lax.axis_index("ep"), lax.axis_index("dp")
    z, x = lax.div(me, 2), lax.rem(me, 2)
    partner = me + 1 - 2 * x
    near = rep + 1 - 2 * lax.rem(rep, 2)
    far = lax.rem(rep + 2, dp_size)
    diagonal = lax.rem(near + 2, dp_size)
    high = lax.div(z, 2)
    middle = lax.div(z * (levels - 1 - z), 2)
    end = (levels - 1) * high
    first_target = middle * end + (1 - middle) * (1 + high)
    second_target = 2 - high

    def level_at(place):
        last = lax.div(place, 3)
        inner = lax.rem(place + 1, 3) * (1 - last) + 3 * last
        low = (1 - middle) * place + middle * inner
        return (1 - high) * low + high * (levels - 1 - low)

    def cols(index, size=chunk):
        return pl.ds(pl.multiple_of(index * size, size), size)

    def rows(index, size):
        return pl.ds(pl.multiple_of(index * size, size), size)

    def raw_copy(tensor, level, index, target, sem):
        return pltpu.make_async_remote_copy(
            src_ref=raw.at[tensor, level, index],
            dst_ref=raw.at[tensor, level, index],
            send_sem=sem,
            recv_sem=raw_recv.at[tensor, level, index],
            device_id={"ep": 2 * target + x},
            device_id_type=MESH,
        )

    def own_copy(tensor, which, index):
        target = first_target if which == 0 else second_target
        return raw_copy(tensor, z, index, target, own_send.at[tensor, which, index])

    def relay_copy(tensor, place, index):
        sem = relay_send.at[tensor, lax.div(place, 2), index]
        return raw_copy(tensor, level_at(place), index, end, sem)

    def cross_copy(tensor, level, index):
        return pltpu.make_async_remote_copy(
            src_ref=cross.at[tensor, level, index],
            dst_ref=slots.at[tensor, rows(2 * level + x, capacity), cols(index)],
            send_sem=cross_send.at[tensor, level, index],
            recv_sem=cross_recv.at[tensor, level, index],
            device_id={"ep": partner},
            device_id_type=MESH,
        )

    def meta_copy(step):
        return pltpu.make_async_remote_copy(
            src_ref=meta.at[me],
            dst_ref=meta.at[me],
            send_sem=meta_send.at[step],
            recv_sem=meta_recv.at[me],
            device_id={"ep": lax.rem(me + step, ep_size)},
            device_id_type=MESH,
        )

    def meta_arrival(step):
        source = lax.rem(me + step, ep_size)
        return pltpu.make_async_remote_copy(
            src_ref=meta.at[source],
            dst_ref=meta.at[source],
            send_sem=meta_send.at[step],
            recv_sem=meta_recv.at[source],
            device_id={"ep": source},
            device_id_type=MESH,
        )

    def dp_copy(source, target, send, recv, peer):
        return pltpu.make_async_remote_copy(
            src_ref=source, dst_ref=target, send_sem=send, recv_sem=recv,
            device_id={"dp": peer}, device_id_type=MESH,
        )

    def pass_copy(unit):
        return dp_copy(
            near_out.at[lax.rem(unit, 2)], near_in.at[unit], pass_send.at[unit], pass_recv.at[unit], near
        )

    def keep_copy(unit):
        return dp_copy(
            keep_out.at[lax.rem(unit, 2)], keep_in.at[unit], keep_send.at[unit], keep_recv.at[unit], near
        )

    def far_copy(unit):
        return dp_copy(near_in.at[unit], far_in.at[unit], far_send.at[unit], far_recv.at[unit], far)

    def return_copy(block):
        return pltpu.make_async_remote_copy(
            src_ref=result.at[rows(block, capacity)],
            dst_ref=back.at[rows(me, capacity)],
            send_sem=ret_send.at[block],
            recv_sem=ret_recv.at[me],
            device_id={"ep": block},
            device_id_type=MESH,
        )

    def prob_copy(block):
        return pltpu.make_async_remote_copy(
            src_ref=prob_out.at[block],
            dst_ref=prob_in.at[me],
            send_sem=prob_send.at[block],
            recv_sem=prob_recv.at[me],
            device_id={"ep": block},
            device_id_type=MESH,
        )

    def return_arrival(source):
        return pltpu.make_async_remote_copy(
            src_ref=result.at[rows(source, capacity)],
            dst_ref=back.at[rows(source, capacity)],
            send_sem=ret_send.at[source],
            recv_sem=ret_recv.at[source],
            device_id={"ep": source},
            device_id_type=MESH,
        )

    def prob_arrival(source):
        return pltpu.make_async_remote_copy(
            src_ref=prob_out.at[source],
            dst_ref=prob_in.at[source],
            send_sem=prob_send.at[source],
            recv_sem=prob_recv.at[source],
            device_id={"ep": source},
            device_id_type=MESH,
        )

    loads = [
        pltpu.make_async_copy(source.at[0], target, load_sem.at[i])
        for i, (source, target) in enumerate(((gate_hbm, w_gate), (up_hbm, w_up), (down_hbm, w_down)))
    ]
    for load in loads:
        load.start()
    for index in range(chunks):
        raw[0, z, index] = tokens_ref[:, index * chunk : (index + 1) * chunk]

    barrier = pltpu.get_barrier_semaphore()
    for step in range(1, ep_size):
        pl.semaphore_signal(
            barrier, inc=1, device_id={"ep": lax.rem(me + step, ep_size)}, device_id_type=MESH
        )
    for peer in (near, far):
        pl.semaphore_signal(barrier, inc=1, device_id={"dp": peer}, device_id_type=MESH)
    pl.semaphore_wait(barrier, ep_size + 1)

    own_copy(0, 0, 0).start()
    scale = jnp.maximum(jnp.max(jnp.abs(grad_ref[...]), axis=1, keepdims=True), 1.0)
    scale_col[...] = scale
    square = (tok_rows, tok_rows)
    eye = lax.broadcasted_iota(jnp.int32, square, 0) == lax.broadcasted_iota(jnp.int32, square, 1)

    def as_row(column):
        return jnp.sum(jnp.where(eye, column, 0.0), axis=0, keepdims=True)

    def as_column(row):
        return jnp.sum(jnp.where(eye, row, 0.0), axis=1, keepdims=True)

    prio_row = prio_ref[...].astype(jnp.float32)
    earlier = jnp.where(as_column(prio_row) < prio_row, 1.0, 0.0).astype(jnp.bfloat16)
    expert_iota = lax.broadcasted_iota(jnp.int32, (ep_size, tok_rows), 0)
    caps = jnp.zeros((ep_size, tok_rows), jnp.float32)
    for expert in range(ep_size):
        caps = jnp.where(expert_iota == expert, caps_ref[expert].astype(jnp.float32), caps)
    matches = [jnp.where(ids_ref[k : k + 1, :] == expert_iota, 1.0, 0.0) for k in range(top)]
    routed = sum(matches[1:], matches[0]).astype(jnp.bfloat16)
    before = jnp.dot(routed, earlier, preferred_element_type=jnp.float32)
    scale_row = as_row(scale)
    for k in range(top):
        rank = jnp.sum(matches[k] * before, axis=0, keepdims=True)
        limit = jnp.sum(matches[k] * caps, axis=0, keepdims=True)
        place = ids_ref[k : k + 1, :].astype(jnp.float32) * capacity + rank
        meta[me, k : k + 1, :] = jnp.where(rank < limit, place, -1.0)
        meta[me, top + k : top + k + 1, :] = probs_ref[k : k + 1, :] * scale_row
    for step in range(1, ep_size):
        meta_copy(step).start()
    for index in range(1, chunks):
        own_copy(0, 0, index).start()
    for index in range(chunks):
        piece = grad_ref[:, index * chunk : (index + 1) * chunk]
        raw[1, z, index] = (piece / scale).astype(jnp.bfloat16)
        own_copy(1, 0, index).start()
    for tensor in range(2):
        for index in range(chunks):
            own_copy(tensor, 1, index).start()
    for k in range(top):
        target_col[k] = as_column(meta[me, k : k + 1, :])
    for load in loads:
        load.wait()
    for step in range(1, ep_size):
        meta_arrival(step).wait_recv()

    slot_iota = lax.broadcasted_iota(jnp.int32, (capacity, tok_rows), 0)

    def slot_names(expert):
        return (slot_iota + expert * capacity).astype(jnp.float32)

    def hits(level, expert):
        table, names = meta[2 * level + x], slot_names(expert)
        total = jnp.zeros((capacity, tok_rows), jnp.float32)
        for k in range(top):
            total = total + jnp.where(table[k : k + 1] == names, 1.0, 0.0)
        return total.astype(jnp.bfloat16)

    def event(tensor, place, index):
        level = level_at(place)

        @pl.when(place > 0)
        def _():
            raw_copy(tensor, level, index, end, relay_send.at[tensor, 0, index]).wait_recv()

        @pl.when(middle * lax.rem(place, 2) == 1)
        def _():
            relay_copy(tensor, place, index).start()

        block = raw[tensor, level, index]
        crossed = jnp.dot(hits(level, partner), block, preferred_element_type=jnp.float32)
        cross[tensor, level, index] = crossed.astype(jnp.bfloat16)
        cross_copy(tensor, level, index).start()
        kept = jnp.dot(hits(level, me), block, preferred_element_type=jnp.float32)
        slots[tensor, rows(2 * level + x, capacity), cols(index)] = kept.astype(jnp.bfloat16)

    def forward_part(place, part):
        level = level_at(place)

        @pl.when(part == 0)
        def _():
            for index in range(chunks):
                cross_copy(0, level, index).wait_recv()
            names = slot_names(me)
            for column in range(2):
                table = meta[2 * level + column]
                total = jnp.zeros((capacity, tok_rows), jnp.float32)
                for k in range(top):
                    total = total + jnp.where(
                        table[k : k + 1] == names, table[top + k : top + k + 1], 0.0
                    )
                weight_col[column * capacity : (column + 1) * capacity, :] = jnp.sum(
                    total, axis=1, keepdims=True
                )

        entries = slots[0, rows(level, group), :]
        gate_pre = contract_last(entries, w_gate[rows(part, chunk), :])
        up_one = contract_last(entries, w_up[rows(part, chunk), :]) + 1.0
        squash = jax.nn.sigmoid(sharpness * gate_pre)
        gated = gate_pre * squash
        activated = up_one * gated
        gated_part[part] = gated
        slope_part[part] = up_one * (squash + sharpness * gated * (1.0 - squash))
        act_part[part] = activated
        deltas[0, rows(level, group), cols(part)] = (activated * weight_col[...]).astype(jnp.bfloat16)

    def backward_part(place, part, wait):
        level = level_at(place)
        if wait:

            @pl.when(part == 0)
            def _():
                for index in range(chunks):
                    cross_copy(1, level, index).wait_recv()

        entries = slots[1, rows(level, group), :]
        back_proj = contract_last(entries, w_down[rows(part, chunk), :])
        act_delta = weight_col[...] * back_proj
        deltas[1, rows(level, group), cols(part)] = (act_delta * slope_part[part]).astype(jnp.bfloat16)
        deltas[2, rows(level, group), cols(part)] = (act_delta * gated_part[part]).astype(jnp.bfloat16)
        slot_sum[part] = jnp.sum(act_part[part] * back_proj, axis=1, keepdims=True)

        @pl.when(part == parts - 1)
        def _():
            total = slot_sum[0]
            for other in range(1, parts):
                total = total + slot_sum[other]
            cap_square = (capacity, tok_rows)
            diagonal_mask = lax.broadcasted_iota(jnp.int32, cap_square, 1) == slot_iota
            for column in range(2):
                line = total[column * capacity : (column + 1) * capacity]
                line = jnp.sum(jnp.where(diagonal_mask, line, 0.0), axis=0, keepdims=True)
                prob_out[2 * level + column] = jnp.broadcast_to(line, prob_out.shape[1:])

    def exchange_step(place, carry):
        def token_step(index, inner):
            event(0, place, index)

            @pl.when(place > 0)
            def _():
                backward_part(place - 1, index, True)

            return inner

        def grad_step(index, inner):
            event(1, place, index)
            forward_part(place, index)
            return inner

        lax.fori_loop(0, chunks, token_step, 0)
        lax.fori_loop(0, chunks, grad_step, 0)
        return carry

    lax.fori_loop(0, levels, exchange_step, 0)

    def send_back():
        def level_step(level, carry):
            def column_step(index, inner):
                total = jnp.dot(
                    deltas[1, rows(level, group), :], w_gate[:, cols(index)],
                    preferred_element_type=jnp.float32,
                ) + jnp.dot(
                    deltas[2, rows(level, group), :], w_up[:, cols(index)],
                    preferred_element_type=jnp.float32,
                )
                result[rows(level, group), cols(index)] = total.astype(jnp.bfloat16)
                return inner

            lax.fori_loop(0, chunks, column_step, 0)
            for column in range(2):
                block = 2 * level + column

                @pl.when(block != me)
                def _():
                    return_copy(block).start()
                    prob_copy(block).start()

                @pl.when(block == me)
                def _():
                    back[rows(me, capacity), :] = result[rows(me, capacity), :]
                    prob_in[me] = prob_out[me]

            return carry

        lax.fori_loop(0, levels, level_step, 0)

    def partial_of(unit, quarter):
        tensor, index = lax.div(unit, chunks), lax.rem(unit, chunks)
        values = slots[1 - lax.div(tensor + 1, 2), :, cols(index)]
        return contract_first(deltas[tensor, :, cols(quarter, share)], values)

    def reduce_step(unit, carry):
        @pl.when(unit < chunks)
        def _():
            cross_copy(1, level_at(levels - 1), lax.rem(unit, chunks)).wait_recv()

        @pl.when(unit == chunks)
        def _():
            def last_step(part, inner):
                backward_part(levels - 1, part, False)
                return inner

            lax.fori_loop(0, parts, last_step, 0)

        @pl.when(unit == chunks + 1)
        def _():
            send_back()

        slot = lax.rem(unit, 2)

        @pl.when(unit >= 2)
        def _():
            pass_copy(unit - 2).wait_send()
            keep_copy(unit - 2).wait_send()

        near_out[slot] = partial_of(unit, diagonal).astype(jnp.bfloat16)
        pass_copy(unit).start()
        passed = partial_of(unit, far)
        pass_copy(unit).wait_recv()
        near_in[unit] = (passed + near_in[unit].astype(jnp.float32)).astype(jnp.bfloat16)
        far_copy(unit).start()
        keep_out[slot] = partial_of(unit, near).astype(jnp.bfloat16)
        keep_copy(unit).start()
        return carry

    lax.fori_loop(0, units, reduce_step, 0)

    def combine():
        for step in range(1, ep_size):
            source = lax.rem(me + step, ep_size)
            return_arrival(source).wait_recv()
            prob_arrival(source).wait_recv()
        shape = (tok_rows, ep_size * capacity)
        names = lax.broadcasted_iota(jnp.int32, shape, 1).astype(jnp.float32)
        table = jnp.zeros(shape, jnp.float32)
        for k in range(top):
            table = table + jnp.where(target_col[k] == names, 1.0, 0.0)
        table = table.astype(jnp.bfloat16)
        for index in range(chunks):
            span = slice(index * chunk, (index + 1) * chunk)
            input_ref[:, span] = jnp.dot(
                table, back[:, span], preferred_element_type=jnp.float32
            ).astype(jnp.bfloat16)
        lane_name = lax.broadcasted_iota(jnp.int32, square, 1).astype(jnp.float32)
        for k in range(top):
            total = jnp.zeros((tok_rows, tok_rows), jnp.float32)
            for expert in range(ep_size):
                found = target_col[k] == lane_name + float(expert * capacity)
                total = total + jnp.where(found, prob_in[expert][:1], 0.0)
            prob_ref[k : k + 1, :] = as_row(scale_col[...] * jnp.sum(total, axis=1, keepdims=True))

    def finish_step(unit, carry):
        @pl.when(unit == units - 2)
        def _():
            combine()

        total = partial_of(unit, rep)
        keep_copy(unit).wait_recv()
        total = total + keep_in[unit].astype(jnp.float32)
        far_copy(unit).wait_recv()
        tensor, index = lax.div(unit, chunks), lax.rem(unit, chunks)
        grads_ref[tensor, :, cols(index)] = (total + far_in[unit].astype(jnp.float32)).astype(
            jnp.bfloat16
        )
        return carry

    lax.fori_loop(0, units, finish_step, 0)

    for tensor in range(2):
        for index in range(chunks):
            own_copy(tensor, 0, index).wait_send()
            own_copy(tensor, 1, index).wait_send()

            @pl.when(middle == 1)
            def _():
                relay_copy(tensor, 1, index).wait_send()
                relay_copy(tensor, 3, index).wait_send()

            for level in range(levels):
                cross_copy(tensor, level, index).wait_send()
    for step in range(1, ep_size):
        meta_copy(step).wait_send()
        peer = lax.rem(me + step, ep_size)
        return_copy(peer).wait_send()
        prob_copy(peer).wait_send()
    for unit in (units - 2, units - 1):
        pass_copy(unit).wait_send()
        keep_copy(unit).wait_send()
    for unit in range(units):
        far_copy(unit).wait_send()


def fused_body(
    grad_out, tokens, probs, expert_ids, priority, cap_counts, gate_weight, up_weight, down_weight
):
    ep_size, dp_size = lax.axis_size("ep"), lax.axis_size("dp")
    tok_rows, width = tokens.shape
    top = expert_ids.shape[1]
    hidden = gate_weight.shape[1]
    capacity = 5 * top * tok_rows // (4 * ep_size)
    slot_rows = ep_size * capacity
    chunk = width // 3
    chunks, parts, levels = width // chunk, hidden // chunk, ep_size // 2
    share = hidden // dp_size
    units = 3 * chunks
    bf16, f32 = jnp.bfloat16, jnp.float32
    vmem, dma = pltpu.VMEM, pltpu.SemaphoreType.DMA
    in_vmem = pl.BlockSpec(memory_space=pltpu.VMEM)
    anywhere = pl.BlockSpec(memory_space=pl.ANY)
    scratch = [
        vmem((hidden, width), bf16), vmem((hidden, width), bf16), vmem((hidden, width), bf16),
        vmem((2, levels, chunks, tok_rows, chunk), bf16),
        vmem((2, slot_rows, width), bf16),
        vmem((2, levels, chunks, capacity, chunk), bf16),
        vmem((3, slot_rows, hidden), bf16),
        vmem((parts, 2 * capacity, chunk), f32),
        vmem((parts, 2 * capacity, chunk), f32),
        vmem((parts, 2 * capacity, chunk), f32),
        vmem((2 * capacity, 1), f32),
        vmem((parts, 2 * capacity, 1), f32),
        vmem((ep_size, 2 * top, tok_rows), f32),
        vmem((top, tok_rows, 1), f32),
        vmem((tok_rows, 1), f32),
        vmem((2, share, chunk), bf16),
        vmem((units, share, chunk), bf16),
        vmem((units, share, chunk), bf16),
        vmem((2, share, chunk), bf16),
        vmem((units, share, chunk), bf16),
        vmem((slot_rows, width), bf16),
        vmem((slot_rows, width), bf16),
        vmem((ep_size, 8, tok_rows), f32),
        vmem((ep_size, 8, tok_rows), f32),
        dma((3,)), dma((2, 2, chunks)), dma((2, 2, chunks)), dma((2, levels, chunks)),
        dma((2, levels, chunks)), dma((2, levels, chunks)), dma((ep_size,)), dma((ep_size,)),
        dma((units,)), dma((units,)), dma((units,)), dma((units,)), dma((units,)), dma((units,)),
        dma((ep_size,)), dma((ep_size,)), dma((ep_size,)), dma((ep_size,)),
    ]
    input_grad, prob_grad, grads = pl.pallas_call(
        functools.partial(fused_kernel, ep_size, dp_size, capacity, chunk),
        out_shape=(
            jax.ShapeDtypeStruct((tok_rows, width), bf16),
            jax.ShapeDtypeStruct((top, tok_rows), f32),
            jax.ShapeDtypeStruct((3, share, width), bf16),
        ),
        in_specs=[in_vmem] * 5 + [pl.BlockSpec(memory_space=pltpu.SMEM)] + [anywhere] * 3,
        out_specs=(in_vmem, in_vmem, in_vmem),
        scratch_shapes=scratch,
        compiler_params=pltpu.CompilerParams(
            collective_id=0, has_side_effects=True, vmem_limit_bytes=66_000_000
        ),
        name="fused_step",
    )(
        tokens, grad_out, probs.T, expert_ids.T, priority, cap_counts, gate_weight, up_weight, down_weight
    )
    return input_grad, prob_grad.T, grads[1][None], grads[2][None], grads[0][None]


def on_device(*arrays):
    return on_device_body(*arrays)


def solution(mesh):
    fused = mesh.shape["ep"] == 8 and mesh.shape["dp"] == 4
    return jax.shard_map(
        fused_body if fused else on_device,
        mesh=mesh,
        in_specs=(
            P(("ep", "dp"), None),
            P(("ep", "dp"), None),
            P(("ep", "dp"), None),
            P(("ep", "dp"), None),
            P(("ep", "dp"), None),
            P(),
            P("ep", None, None),
            P("ep", None, None),
            P("ep", None, None),
        ),
        out_specs=(
            P(("ep", "dp"), None),
            P(("ep", "dp"), None),
            P("ep", "dp", None),
            P("ep", "dp", None),
            P("ep", "dp", None),
        ),
        check_vma=False,
    )
```

```python
import functools

import jax
import jax.numpy as jnp
from jax import lax
from jax.experimental import pallas as pl
from jax.experimental.pallas import tpu as pltpu
from jax.sharding import PartitionSpec as P


sharpness = 1.702


def contract_last(first_op, second_op):
    return lax.dot_general(
        first_op, second_op, (((1,), (1,)), ((), ())), preferred_element_type=jnp.float32
    )


def contract_first(first_op, second_op):
    return lax.dot_general(
        first_op, second_op, (((0,), (0,)), ((), ())), preferred_element_type=jnp.float32
    )


def route_table(expert_ids, priority, cap_counts, buckets, capacity):
    ranking = priority[0]
    earlier = (ranking[None, :] < ranking[:, None]).astype(jnp.bfloat16)
    expert_range = lax.broadcasted_iota(jnp.int32, (1, 1, buckets), 2)
    matches = (expert_ids[:, :, None] == expert_range).astype(jnp.float32)
    routed = jnp.sum(matches, axis=1).astype(jnp.bfloat16)
    before = jnp.dot(earlier, routed, preferred_element_type=jnp.float32)
    slot_rank = jnp.sum(matches * before[:, None, :], axis=2).astype(jnp.int32)
    keep_limit = jnp.sum(matches * cap_counts.astype(jnp.float32)[None, None, :], axis=2)
    kept = slot_rank < keep_limit.astype(jnp.int32)
    return jnp.where(kept, expert_ids * capacity + slot_rank, -1)


def exchange_dispatch(tokens, quantized, pair_weight, placement, ep_size, capacity):
    table = jnp.any(placement, axis=1).astype(jnp.bfloat16)
    bucket_shape = (ep_size, capacity, tokens.shape[1])
    send_x = contract_first(table, tokens).astype(jnp.bfloat16)
    send_q = contract_first(table, quantized).astype(jnp.bfloat16)
    send_weight = jnp.sum(jnp.where(placement, pair_weight[:, :, None], 0.0), axis=(0, 1))
    slot_x = exchange(send_x.reshape(bucket_shape), "ep").reshape(-1, tokens.shape[1])
    slot_q = exchange(send_q.reshape(bucket_shape), "ep").reshape(-1, tokens.shape[1])
    weight = exchange(send_weight.reshape(ep_size, capacity), "ep").reshape(-1)
    return slot_x, slot_q, weight


def relay_dispatch(tokens, quantized, target, pair_weight, capacity):
    ep_size, levels = lax.axis_size("ep"), lax.axis_size("ep") // 2
    me = lax.axis_index("ep")
    z, x = me // 2, me % 2
    meta = jnp.concatenate([target.astype(jnp.float32).T, pair_weight.T], axis=0)
    table = exchange(jnp.broadcast_to(meta[None], (ep_size, *meta.shape)), "ep")
    top = target.shape[1]
    slots = lax.broadcasted_iota(jnp.int32, (1, capacity, 1), 1).astype(jnp.float32)

    def hop(array, step, sign):
        sources = [h for h in range(levels) if 0 <= h - sign * (step - 1) < levels and 0 <= h + sign < levels]
        return lax.ppermute(
            array, "ep", [(2 * h + j, 2 * (h + sign) + j) for h in sources for j in range(2)]
        )

    def hit(block, expert):
        rows = lax.dynamic_index_in_dim(table, block, 0, keepdims=False)[:top]
        base = (expert * capacity).astype(jnp.float32)
        return jnp.any(rows[:, None, :] == slots + base, axis=0).astype(jnp.bfloat16)

    second = jnp.where(z == 0, 1, z - 1)
    third = jnp.where(z < 2, z + 2, z - 2)
    fourth = jnp.where(z == 0, 3, jnp.where(z == 1, 2, jnp.where(z == 2, 3, 0)))
    order = (z, second, third, fourth)
    own_hits = [hit(2 * h + x, me) for h in order]
    cross_hits = [hit(2 * h + x, me ^ 1) for h in order]
    inner = (z == 1) | (z == 2)

    def pick(hits, rows):
        return jnp.dot(hits, rows, preferred_element_type=jnp.float32).astype(jnp.bfloat16)

    def spread(block):
        up_one, down_one = hop(block, 1, 1), hop(block, 1, -1)
        up_two, down_two = hop(up_one, 2, 1), hop(down_one, 2, -1)
        up_three, down_three = hop(up_two, 3, 1), hop(down_two, 3, -1)
        held = (
            block,
            jnp.where(z == 0, down_one, up_one),
            jnp.where(z < 2, down_two, up_two),
            jnp.where(inner, down_one, jnp.where(z == 0, down_three, up_three)),
        )
        out = jnp.zeros((ep_size * capacity, block.shape[1]), jnp.bfloat16)
        for i in range(4):
            crossed = lax.ppermute(
                pick(cross_hits[i], held[i]), "ep", [(d, d ^ 1) for d in range(ep_size)]
            )
            kept_here = pick(own_hits[i], held[i])
            base = 2 * order[i]
            out = lax.dynamic_update_slice_in_dim(out, kept_here, (base + x) * capacity, 0)
            out = lax.dynamic_update_slice_in_dim(out, crossed, (base + 1 - x) * capacity, 0)
        return out, (up_one, down_one)

    slot_x, arrived = spread(tokens)
    quantized, _ = lax.optimization_barrier((quantized, arrived))
    slot_q, _ = spread(quantized)
    targets = table[:, :top, None, :]
    base = (me * capacity).astype(jnp.float32)
    weight = jnp.sum(
        jnp.where(targets == slots[None] + base, table[:, top:, None, :], 0.0), axis=(1, 3)
    )
    return slot_x, slot_q, weight.reshape(-1)


def exchange(array, axis):
    return lax.all_to_all(array, axis, split_axis=0, concat_axis=0, tiled=True)


def pair_scatter(deltas, values, after=None):
    dp_size = lax.axis_size("dp")
    hidden = deltas.shape[1]
    if dp_size != 4:
        part = contract_first(deltas, values).astype(jnp.bfloat16)
        return lax.psum_scatter(part, "dp", scatter_dimension=0, tiled=True), part
    share = hidden // dp_size
    me = lax.axis_index("dp")
    near, far = me ^ 1, me ^ 2

    def quarter(which):
        columns = lax.dynamic_slice_in_dim(deltas, which * share, share, 1)
        return contract_first(columns, values)

    def swap(array, bit):
        return lax.ppermute(array, "dp", [(i, i ^ bit) for i in range(dp_size)])

    from_near_far = swap(quarter(near ^ 2).astype(jnp.bfloat16), 1)
    from_near_own = swap(quarter(near).astype(jnp.bfloat16), 1)
    passed = (quarter(far) + from_near_far.astype(jnp.float32)).astype(jnp.bfloat16)
    from_far = swap(passed, 2)
    if after is not None:
        from_far, _ = lax.optimization_barrier((from_far, after))
    own = quarter(me) + from_near_own.astype(jnp.float32)
    return (own + from_far.astype(jnp.float32)).astype(jnp.bfloat16), passed


def on_device_body(
    grad_out, tokens, probs, expert_ids, priority, cap_counts, gate_weight, up_weight, down_weight
):
    ep_size = lax.axis_size("ep")
    tok_rows, model_width = tokens.shape
    route_count = expert_ids.shape[1]
    capacity = 5 * route_count * tok_rows // (4 * ep_size)
    slot_rows = ep_size * capacity
    bucket_shape = (ep_size, capacity, model_width)
    target = route_table(expert_ids, priority, cap_counts, ep_size, capacity)
    slot_range = lax.broadcasted_iota(jnp.int32, (1, 1, slot_rows), 2)
    placement = target[:, :, None] == slot_range
    row_scale = jnp.maximum(jnp.max(jnp.abs(grad_out), axis=1), 1.0)
    quantized = (grad_out / row_scale[:, None]).astype(jnp.bfloat16)
    pair_weight = probs * row_scale[:, None]
    if ep_size == 8:
        slot_x, slot_q, weight = relay_dispatch(tokens, quantized, target, pair_weight, capacity)
    else:
        slot_x, slot_q, weight = exchange_dispatch(
            tokens, quantized, pair_weight, placement, ep_size, capacity
        )
    weight = weight[:, None]
    w_gate = gate_weight[0]
    w_up = up_weight[0]
    w_down = down_weight[0]

    gate_pre = contract_last(slot_x, w_gate)
    up_pre = contract_last(slot_x, w_up)
    squash = jax.nn.sigmoid(sharpness * gate_pre)
    gated = gate_pre * squash
    activated = (up_pre + 1.0) * gated
    act_scaled = (activated * weight).astype(jnp.bfloat16)
    down_share, passed = pair_scatter(act_scaled, slot_q)
    later_q, _ = lax.optimization_barrier((slot_q, passed))
    back_proj = contract_last(later_q, w_down)
    act_delta = weight * back_proj
    up_delta = (act_delta * gated).astype(jnp.bfloat16)
    gate_delta = (
        act_delta * (up_pre + 1.0) * (squash + sharpness * gate_pre * squash * (1.0 - squash))
    ).astype(jnp.bfloat16)
    slot_out = jnp.sum(activated * back_proj, axis=1)
    gate_share, _ = pair_scatter(gate_delta, slot_x)
    up_share, _ = pair_scatter(up_delta, slot_x, gate_share)
    in_delta = jnp.dot(gate_delta, w_gate, preferred_element_type=jnp.float32) + jnp.dot(
        up_delta, w_up, preferred_element_type=jnp.float32
    )
    slot_in = in_delta.astype(jnp.bfloat16)
    back_in = exchange(slot_in.reshape(bucket_shape), "ep").reshape(slot_rows, model_width)
    back_prob = exchange(slot_out.reshape(ep_size, capacity), "ep").reshape(slot_rows)
    prob_grad = row_scale[:, None] * jnp.sum(
        jnp.where(placement, back_prob[None, None, :], 0.0), axis=2
    )
    table_low = jnp.any(placement, axis=1).astype(jnp.bfloat16)
    input_grad = jnp.dot(table_low, back_in, preferred_element_type=jnp.float32).astype(
        jnp.bfloat16
    )
    return (input_grad, prob_grad, gate_share[None], up_share[None], down_share[None])


MESH = pl.DeviceIdType.MESH


def fused_kernel(
    ep_size, dp_size, capacity, chunk,
    tokens_ref, grad_ref, probs_ref, ids_ref, prio_ref, caps_ref, gate_hbm, up_hbm, down_hbm,
    input_ref, prob_ref, grads_ref,
    w_gate, w_up, w_down, raw, slots, cross, deltas, act_part, weight_col,
    slot_sum, meta, target_col, scale_col, keep_out, keep_in, result, back, prob_out, prob_in,
    far_slots, far_deltas, far_weight, far_meta,
    load_sem, own_send, relay_send, raw_recv, cross_send, cross_recv, meta_send, meta_recv,
    keep_send, keep_recv, ret_send, ret_recv, prob_send, prob_recv,
    slot_send, slot_recv, side_send, side_recv, table_send, table_recv,
):
    tok_rows, width = tokens_ref.shape
    top = ids_ref.shape[0]
    hidden = w_gate.shape[0]
    share = hidden // dp_size
    chunks = width // chunk
    levels = ep_size // 2
    group = 2 * capacity
    pair = 2 * group
    units = 3
    me, rep = lax.axis_index("ep"), lax.axis_index("dp")
    z, x = lax.div(me, 2), lax.rem(me, 2)
    partner = me + 1 - 2 * x
    near = rep + 1 - 2 * lax.rem(rep, 2)
    far = lax.rem(rep + 2, dp_size)
    diagonal = lax.rem(near + 2, dp_size)
    high = lax.div(z, 2)
    middle = lax.div(z * (levels - 1 - z), 2)
    end = (levels - 1) * high
    first_target = middle * end + (1 - middle) * (1 + high)
    second_target = 2 - high

    def level_at(place):
        last = lax.div(place, 3)
        inner = lax.rem(place + 1, 3) * (1 - last) + 3 * last
        low = (1 - middle) * place + middle * inner
        return (1 - high) * low + high * (levels - 1 - low)

    def cols(index, size=chunk):
        return pl.ds(pl.multiple_of(index * size, size), size)

    def rows(index, size):
        return pl.ds(pl.multiple_of(index * size, size), size)

    def remote(source, target, send, recv, peer):
        return pltpu.make_async_remote_copy(
            src_ref=source, dst_ref=target, send_sem=send, recv_sem=recv,
            device_id=peer, device_id_type=MESH,
        )

    def raw_copy(tensor, level, index, target, sem):
        block = raw.at[tensor, level, index]
        return remote(block, block, sem, raw_recv.at[tensor, level, index], {"ep": 2 * target + x})

    def own_copy(tensor, which, index):
        target = first_target if which == 0 else second_target
        return raw_copy(tensor, z, index, target, own_send.at[tensor, which, index])

    def relay_copy(tensor, place, index):
        sem = relay_send.at[tensor, lax.div(place, 2), index]
        return raw_copy(tensor, level_at(place), index, end, sem)

    def cross_copy(tensor, place, index):
        return remote(
            cross.at[tensor, lax.rem(place, 2), index],
            slots.at[tensor, rows(2 * place + x, capacity), cols(index)],
            cross_send.at[tensor, place, index], cross_recv.at[tensor, place, index],
            {"ep": partner},
        )

    def meta_copy(step):
        peer = lax.rem(me + step, ep_size)
        return remote(meta.at[me], meta.at[me], meta_send.at[step], meta_recv.at[me], {"ep": peer})

    def meta_arrival(step):
        peer = lax.rem(me + step, ep_size)
        table = meta.at[peer]
        return remote(table, table, meta_send.at[step], meta_recv.at[peer], {"ep": peer})

    def table_copy(which):
        peer = far if which == 0 else diagonal
        return remote(
            meta, far_meta.at[which], table_send.at[which], table_recv.at[which], {"dp": peer}
        )

    def keep_copy(unit):
        return remote(
            keep_out, keep_in.at[unit], keep_send.at[unit], keep_recv.at[unit],
            {"dp": near},
        )

    def far_rows(place, which):
        return pl.ds(pl.multiple_of(which * pair + lax.rem(place, 2) * group, group), group)

    def slot_copy(tensor, place, column):
        start = lax.rem(place, 2) * group + column * capacity
        return remote(
            slots.at[tensor, rows(2 * place + column, capacity)],
            far_slots.at[
                tensor, lax.div(place, 2), pl.ds(pl.multiple_of(start, capacity), capacity)
            ],
            slot_send.at[tensor, place, column], slot_recv.at[tensor, place, column], {"dp": far},
        )

    def side_copy(tensor, place):
        return remote(
            far_slots.at[tensor, lax.div(place, 2), far_rows(place, 0)],
            far_slots.at[tensor, lax.div(place, 2), far_rows(place, 1)],
            side_send.at[tensor, place], side_recv.at[tensor, place], {"dp": near},
        )

    def return_copy(place, column, block):
        return remote(
            result.at[rows(2 * place + column, capacity)], back.at[rows(me, capacity)],
            ret_send.at[place, column], ret_recv.at[me], {"ep": block},
        )

    def prob_copy(place, column, block):
        return remote(
            prob_out.at[place, column], prob_in.at[me],
            prob_send.at[place, column], prob_recv.at[me], {"ep": block},
        )

    def return_arrival(source):
        span = back.at[rows(source, capacity)]
        return remote(span, span, ret_send.at[0, 0], ret_recv.at[source], {"ep": source})

    def prob_arrival(source):
        span = prob_in.at[source]
        return remote(span, span, prob_send.at[0, 0], prob_recv.at[source], {"ep": source})

    loads = [
        pltpu.make_async_copy(source.at[0], target, load_sem.at[i])
        for i, (source, target) in enumerate(((gate_hbm, w_gate), (up_hbm, w_up), (down_hbm, w_down)))
    ]
    for load in loads:
        load.start()
    for index in range(chunks):
        raw[0, z, index] = tokens_ref[:, index * chunk : (index + 1) * chunk]

    barrier = pltpu.get_barrier_semaphore()
    for step in range(1, ep_size):
        pl.semaphore_signal(
            barrier, inc=1, device_id={"ep": lax.rem(me + step, ep_size)}, device_id_type=MESH
        )
    for peer in (near, far, diagonal):
        pl.semaphore_signal(barrier, inc=1, device_id={"dp": peer}, device_id_type=MESH)
    pl.semaphore_wait(barrier, ep_size + 2)

    own_copy(0, 0, 0).start()
    scale = jnp.maximum(jnp.max(jnp.abs(grad_ref[...]), axis=1, keepdims=True), 1.0)
    scale_col[...] = scale
    square = (tok_rows, tok_rows)
    eye = lax.broadcasted_iota(jnp.int32, square, 0) == lax.broadcasted_iota(jnp.int32, square, 1)

    def as_row(column):
        return jnp.sum(jnp.where(eye, column, 0.0), axis=0, keepdims=True)

    def as_column(row):
        return jnp.sum(jnp.where(eye, row, 0.0), axis=1, keepdims=True)

    prio_row = prio_ref[...].astype(jnp.float32)
    earlier = jnp.where(as_column(prio_row) < prio_row, 1.0, 0.0).astype(jnp.bfloat16)
    expert_iota = lax.broadcasted_iota(jnp.int32, (ep_size, tok_rows), 0)
    caps = jnp.zeros((ep_size, tok_rows), jnp.float32)
    for expert in range(ep_size):
        caps = jnp.where(expert_iota == expert, caps_ref[expert].astype(jnp.float32), caps)
    matches = [jnp.where(ids_ref[k : k + 1, :] == expert_iota, 1.0, 0.0) for k in range(top)]
    routed = sum(matches[1:], matches[0]).astype(jnp.bfloat16)
    before = jnp.dot(routed, earlier, preferred_element_type=jnp.float32)
    scale_row = as_row(scale)
    for k in range(top):
        rank = jnp.sum(matches[k] * before, axis=0, keepdims=True)
        limit = jnp.sum(matches[k] * caps, axis=0, keepdims=True)
        place = ids_ref[k : k + 1, :].astype(jnp.float32) * capacity + rank
        meta[me, k : k + 1, :] = jnp.where(rank < limit, place, -1.0)
        meta[me, top + k : top + k + 1, :] = probs_ref[k : k + 1, :] * scale_row
    for step in range(1, ep_size):
        meta_copy(step).start()
    for index in range(1, chunks):
        own_copy(0, 0, index).start()
    for index in range(chunks):
        piece = grad_ref[:, index * chunk : (index + 1) * chunk]
        raw[1, z, index] = (piece / scale).astype(jnp.bfloat16)
        own_copy(1, 0, index).start()
    for tensor in range(2):
        for index in range(chunks):
            own_copy(tensor, 1, index).start()
    for k in range(top):
        target_col[k] = as_column(meta[me, k : k + 1, :])

    slot_iota = lax.broadcasted_iota(jnp.int32, (capacity, tok_rows), 0)

    def slot_names(expert):
        return (slot_iota + expert * capacity).astype(jnp.float32)

    def hits(level, expert):
        table, names = meta[2 * level + x], slot_names(expert)
        total = jnp.zeros((capacity, tok_rows), jnp.float32)
        for k in range(top):
            total = total + jnp.where(table[k : k + 1] == names, 1.0, 0.0)
        return total.astype(jnp.bfloat16)

    def weight_of(table):
        names = slot_names(me)
        total = jnp.zeros((capacity, tok_rows), jnp.float32)
        for k in range(top):
            total = total + jnp.where(table[k : k + 1] == names, table[top + k : top + k + 1], 0.0)
        return jnp.sum(total, axis=1, keepdims=True)

    def event(tensor, place, index):
        level = level_at(place)

        @pl.when(place > 0)
        def _():
            raw_copy(tensor, level, index, end, relay_send.at[tensor, 0, index]).wait_recv()

        @pl.when(middle * lax.rem(place, 2) == 1)
        def _():
            relay_copy(tensor, place, index).start()

        @pl.when(place > 1)
        def _():
            cross_copy(tensor, place - 2, index).wait_send()

        block = raw[tensor, level, index]
        crossed = jnp.dot(hits(level, partner), block, preferred_element_type=jnp.float32)
        cross[tensor, lax.rem(place, 2), index] = crossed.astype(jnp.bfloat16)
        cross_copy(tensor, place, index).start()
        kept = jnp.dot(hits(level, me), block, preferred_element_type=jnp.float32)
        slots[tensor, rows(2 * place + x, capacity), cols(index)] = kept.astype(jnp.bfloat16)

        @pl.when(index == chunks - 1)
        def _():
            slot_copy(tensor, place, x).start()

    def share_slots(tensor, place):
        for index in range(chunks):
            cross_copy(tensor, place, index).wait_recv()
        slot_copy(tensor, place, 1 - x).start()

    def activate(gate_pre, up_pre):
        up_one = up_pre + 1.0
        squash = jax.nn.sigmoid(sharpness * gate_pre)
        gated = gate_pre * squash
        return gated, up_one * (squash + sharpness * gated * (1.0 - squash)), up_one * gated

    def forward_part(first, count, part):
        @pl.when(part == 0)
        def _():
            for inner in range(count):
                for column in range(2):
                    base = inner * group + column * capacity
                    table = meta[2 * level_at(first + inner) + column]
                    weight_col[base : base + capacity, :] = weight_of(table)

        size = count * group
        span = pl.ds(pl.multiple_of(first * group, group), size)
        entries = slots[0, span, :]
        gate_pre = contract_last(entries, w_gate[rows(part, chunk), :])
        up_pre = contract_last(entries, w_up[rows(part, chunk), :])
        gated, slope, activated = activate(gate_pre, up_pre)
        deltas[1, span, cols(part)] = slope.astype(jnp.bfloat16)
        deltas[2, span, cols(part)] = gated.astype(jnp.bfloat16)
        act_part[part, :size] = activated.astype(jnp.bfloat16)
        deltas[0, span, cols(part)] = (activated * weight_col[:size]).astype(jnp.bfloat16)

    def backward_part(first, count, part):
        size = count * group
        span = pl.ds(pl.multiple_of(first * group, group), size)
        back_proj = contract_last(slots[1, span, :], w_down[rows(part, chunk), :])
        act_delta = weight_col[:size] * back_proj
        for kind in (1, 2):
            stored = deltas[kind, span, cols(part)]
            deltas[kind, span, cols(part)] = (act_delta * stored).astype(jnp.bfloat16)
        slot_sum[part, :size] = jnp.sum(act_part[part, :size] * back_proj, axis=1, keepdims=True)

        @pl.when(part == chunks - 1)
        def _():
            total = slot_sum[0, :size]
            for other in range(1, chunks):
                total = total + slot_sum[other, :size]
            cap_square = (capacity, tok_rows)
            mask = lax.broadcasted_iota(jnp.int32, cap_square, 1) == slot_iota
            for inner in range(count):
                for column in range(2):
                    base = inner * group + column * capacity
                    line = jnp.sum(
                        jnp.where(mask, total[base : base + capacity], 0.0), axis=0, keepdims=True
                    )
                    prob_out[first + inner, column] = jnp.broadcast_to(line, prob_out.shape[2:])

    def return_part(first, count, part):
        span = pl.ds(pl.multiple_of(first * group, group), count * group)
        total = jnp.dot(
            deltas[1, span, :], w_gate[:, cols(part)], preferred_element_type=jnp.float32
        ) + jnp.dot(deltas[2, span, :], w_up[:, cols(part)], preferred_element_type=jnp.float32)
        result[span, cols(part)] = total.astype(jnp.bfloat16)

        @pl.when((part == chunks - 1) & ((first == 0) | (middle == 0)))
        def _():
            send_back(first, count)

    def send_back(first, count):
        for inner in range(count):
            place = first + count - 1 - inner
            for column in range(2):
                block = 2 * level_at(place) + column

                @pl.when(block != me)
                def _():
                    return_copy(place, column, block).start()
                    prob_copy(place, column, block).start()

                @pl.when(block == me)
                def _():
                    back[rows(me, capacity), :] = result[rows(2 * place + column, capacity), :]
                    prob_in[me] = prob_out[place, column]

    period = 4 * chunks

    def main_step(step, carry):
        @pl.when(step == 2 * chunks)
        def _():
            for hop in range(1, ep_size):
                meta_arrival(hop).wait_recv()
            for which in range(2):
                table_copy(which).start()
            for load in loads:
                load.wait()

        @pl.when(step < 2 * period)
        def _():
            item = lax.div(step, chunks)
            event(lax.rem(item, 2), lax.div(item, 2), lax.rem(step, chunks))

        late = step - chunks - 1

        @pl.when((late >= 0) & (lax.rem(late + period, chunks) == 0))
        def _():
            item = lax.div(late, chunks)

            @pl.when(item < 2 * levels)
            def _():
                share_slots(lax.rem(item, 2), lax.div(item, 2))

        for number, task in enumerate((forward_part, backward_part, return_part)):
            since = step - (3 + number) * chunks - 1

            @pl.when((since >= 0) & (lax.rem(since + 2 * period, period) < chunks))
            def _():
                task(2 * lax.div(since, period), 2, lax.rem(since, period))

        return carry

    lax.fori_loop(0, 2 * period + 2 * chunks + 1, main_step, 0)

    def keep_step(unit, carry):
        total = partial_of(unit, near).astype(jnp.bfloat16)

        @pl.when(unit >= 1)
        def _():
            keep_copy(unit - 1).wait_send()

        keep_out[...] = total
        keep_copy(unit).start()
        return carry

    def partial_of(unit, quarter):
        return contract_first(deltas[unit, :, cols(quarter, share)], slots[1 - lax.div(unit + 1, 2)])

    def far_partial(unit, half):
        return contract_first(far_deltas[unit], far_slots[1 - lax.div(unit + 1, 2), half])

    def pull(tensor, half):
        for inner in range(2):
            for column in range(2):
                slot_copy(tensor, 2 * half + inner, column).wait_recv()
            side_copy(tensor, 2 * half + inner).start()

    def settle(tensor, half):
        for inner in range(2):
            side_copy(tensor, 2 * half + inner).wait_recv()

    def far_forward(half):
        for which in range(2):
            for inner in range(2):
                for column in range(2):
                    base = which * pair + inner * group + column * capacity
                    table = far_meta[which, 2 * level_at(2 * half + inner) + column]
                    far_weight[base : base + capacity, :] = weight_of(table)
        entries = far_slots[0, half]
        gate_pre = contract_last(entries, w_gate[rows(rep, share), :])
        up_pre = contract_last(entries, w_up[rows(rep, share), :])
        gated, slope, activated = activate(gate_pre, up_pre)
        far_deltas[1] = slope.astype(jnp.bfloat16)
        far_deltas[2] = gated.astype(jnp.bfloat16)
        far_deltas[0] = (activated * far_weight[...]).astype(jnp.bfloat16)

    def far_backward(half):
        back_proj = contract_last(far_slots[1, half], w_down[rows(rep, share), :])
        act_delta = far_weight[...] * back_proj
        for kind in (1, 2):
            far_deltas[kind] = (act_delta * far_deltas[kind]).astype(jnp.bfloat16)

    def combine():
        for step in range(1, ep_size):
            source = lax.rem(me + step, ep_size)
            return_arrival(source).wait_recv()
            prob_arrival(source).wait_recv()
        shape = (tok_rows, ep_size * capacity)
        names = lax.broadcasted_iota(jnp.int32, shape, 1).astype(jnp.float32)
        table = jnp.zeros(shape, jnp.float32)
        for k in range(top):
            table = table + jnp.where(target_col[k] == names, 1.0, 0.0)
        table = table.astype(jnp.bfloat16)
        for index in range(chunks):
            span = slice(index * chunk, (index + 1) * chunk)
            input_ref[:, span] = jnp.dot(
                table, back[:, span], preferred_element_type=jnp.float32
            ).astype(jnp.bfloat16)
        lane_name = lax.broadcasted_iota(jnp.int32, square, 1).astype(jnp.float32)
        for k in range(top):
            total = jnp.zeros((tok_rows, tok_rows), jnp.float32)
            for expert in range(ep_size):
                found = target_col[k] == lane_name + float(expert * capacity)
                total = total + jnp.where(found, prob_in[expert][:1], 0.0)
            prob_ref[k : k + 1, :] = as_row(scale_col[...] * jnp.sum(total, axis=1, keepdims=True))

    def far_step(half, carry):
        @pl.when(half == 0)
        def _():
            pull(0, 0)
            pull(1, 0)
            for which in range(2):
                table_copy(which).wait_recv()
            lax.fori_loop(0, units, keep_step, 0)

        settle(0, half)
        far_forward(half)

        settle(1, half)
        far_backward(half)

        @pl.when((half == 0) & (middle == 1))
        def _():
            send_back(2, 2)

        def grads_step(unit, inner):
            total = far_partial(unit, half)

            @pl.when((half == 0) & (unit > 0))
            def _():
                pull(unit - 1, 1)

            @pl.when(half == 0)
            def _():
                first = total + partial_of(unit, rep)
                keep_copy(unit).wait_recv()
                grads_ref[unit] = (first + keep_in[unit].astype(jnp.float32)).astype(jnp.bfloat16)

            @pl.when(half == 1)
            def _():
                grads_ref[unit] = (total + grads_ref[unit].astype(jnp.float32)).astype(jnp.bfloat16)

            return inner

        lax.fori_loop(0, units, grads_step, 0)
        return carry

    lax.fori_loop(0, 2, far_step, 0)
    combine()

    for tensor in range(2):
        for index in range(chunks):
            own_copy(tensor, 0, index).wait_send()
            own_copy(tensor, 1, index).wait_send()

            @pl.when(middle == 1)
            def _():
                relay_copy(tensor, 1, index).wait_send()
                relay_copy(tensor, 3, index).wait_send()

            for place in range(2, levels):
                cross_copy(tensor, place, index).wait_send()
        for place in range(levels):
            for column in range(2):
                slot_copy(tensor, place, column).wait_send()
            side_copy(tensor, place).wait_send()
    for step in range(1, ep_size):
        meta_copy(step).wait_send()
    for place in range(levels):
        for column in range(2):
            block = 2 * level_at(place) + column

            @pl.when(block != me)
            def _():
                return_copy(place, column, block).wait_send()
                prob_copy(place, column, block).wait_send()

    keep_copy(units - 1).wait_send()
    for which in range(2):
        table_copy(which).wait_send()


def fused_body(
    grad_out, tokens, probs, expert_ids, priority, cap_counts, gate_weight, up_weight, down_weight
):
    ep_size, dp_size = lax.axis_size("ep"), lax.axis_size("dp")
    tok_rows, width = tokens.shape
    top = expert_ids.shape[1]
    hidden = gate_weight.shape[1]
    capacity = 5 * top * tok_rows // (4 * ep_size)
    slot_rows = ep_size * capacity
    pair = slot_rows // 2
    chunk = width // 3
    chunks, levels = width // chunk, ep_size // 2
    share = hidden // dp_size
    units = 3
    bf16, f32 = jnp.bfloat16, jnp.float32
    vmem, dma = pltpu.VMEM, pltpu.SemaphoreType.DMA
    in_vmem = pl.BlockSpec(memory_space=pltpu.VMEM)
    anywhere = pl.BlockSpec(memory_space=pl.ANY)
    scratch = [
        vmem((hidden, width), bf16), vmem((hidden, width), bf16), vmem((hidden, width), bf16),
        vmem((2, levels, chunks, tok_rows, chunk), bf16),
        vmem((2, slot_rows, width), bf16),
        vmem((2, 2, chunks, capacity, chunk), bf16),
        vmem((3, slot_rows, hidden), bf16),
        vmem((chunks, pair, chunk), bf16),
        vmem((pair, 1), f32),
        vmem((chunks, pair, 1), f32),
        vmem((ep_size, 2 * top, tok_rows), f32),
        vmem((top, tok_rows, 1), f32),
        vmem((tok_rows, 1), f32),
        vmem((share, width), bf16),
        vmem((units, share, width), bf16),
        vmem((slot_rows, width), bf16),
        vmem((slot_rows, width), bf16),
        vmem((levels, 2, 8, tok_rows), f32),
        vmem((ep_size, 8, tok_rows), f32),
        vmem((2, 2, 2 * pair, width), bf16),
        vmem((3, 2 * pair, share), bf16),
        vmem((2 * pair, 1), f32),
        vmem((2, ep_size, 2 * top, tok_rows), f32),
        dma((3,)), dma((2, 2, chunks)), dma((2, 2, chunks)), dma((2, levels, chunks)),
        dma((2, levels, chunks)), dma((2, levels, chunks)), dma((ep_size,)), dma((ep_size,)),
        dma((units,)), dma((units,)), dma((levels, 2)), dma((ep_size,)), dma((levels, 2)),
        dma((ep_size,)), dma((2, levels, 2)), dma((2, levels, 2)), dma((2, levels)), dma((2, levels)),
        dma((2,)), dma((2,)),
    ]
    input_grad, prob_grad, grads = pl.pallas_call(
        functools.partial(fused_kernel, ep_size, dp_size, capacity, chunk),
        out_shape=(
            jax.ShapeDtypeStruct((tok_rows, width), bf16),
            jax.ShapeDtypeStruct((top, tok_rows), f32),
            jax.ShapeDtypeStruct((3, share, width), bf16),
        ),
        in_specs=[in_vmem] * 5 + [pl.BlockSpec(memory_space=pltpu.SMEM)] + [anywhere] * 3,
        out_specs=(in_vmem, in_vmem, in_vmem),
        scratch_shapes=scratch,
        compiler_params=pltpu.CompilerParams(
            collective_id=0, has_side_effects=True, vmem_limit_bytes=66_000_000
        ),
        name="fused_step",
    )(
        tokens, grad_out, probs.T, expert_ids.T, priority, cap_counts, gate_weight, up_weight, down_weight
    )
    return input_grad, prob_grad.T, grads[1][None], grads[2][None], grads[0][None]


def on_device(*arrays):
    return on_device_body(*arrays)


def solution(mesh):
    fused = mesh.shape["ep"] == 8 and mesh.shape["dp"] == 4
    return jax.shard_map(
        fused_body if fused else on_device,
        mesh=mesh,
        in_specs=(
            P(("ep", "dp"), None),
            P(("ep", "dp"), None),
            P(("ep", "dp"), None),
            P(("ep", "dp"), None),
            P(("ep", "dp"), None),
            P(),
            P("ep", None, None),
            P("ep", None, None),
            P("ep", None, None),
        ),
        out_specs=(
            P(("ep", "dp"), None),
            P(("ep", "dp"), None),
            P("ep", "dp", None),
            P("ep", "dp", None),
            P("ep", "dp", None),
        ),
        check_vma=False,
    )
```

```python
import functools

import jax
import jax.numpy as jnp
from jax import lax
from jax.experimental import pallas as pl
from jax.experimental.pallas import tpu as pltpu
from jax.sharding import PartitionSpec as P


sharpness = 1.702


def contract_last(first_op, second_op):
    return lax.dot_general(
        first_op, second_op, (((1,), (1,)), ((), ())), preferred_element_type=jnp.float32
    )


def contract_first(first_op, second_op):
    return lax.dot_general(
        first_op, second_op, (((0,), (0,)), ((), ())), preferred_element_type=jnp.float32
    )


def route_table(expert_ids, priority, cap_counts, buckets, capacity):
    ranking = priority[0]
    earlier = (ranking[None, :] < ranking[:, None]).astype(jnp.bfloat16)
    expert_range = lax.broadcasted_iota(jnp.int32, (1, 1, buckets), 2)
    matches = (expert_ids[:, :, None] == expert_range).astype(jnp.float32)
    routed = jnp.sum(matches, axis=1).astype(jnp.bfloat16)
    before = jnp.dot(earlier, routed, preferred_element_type=jnp.float32)
    slot_rank = jnp.sum(matches * before[:, None, :], axis=2).astype(jnp.int32)
    keep_limit = jnp.sum(matches * cap_counts.astype(jnp.float32)[None, None, :], axis=2)
    kept = slot_rank < keep_limit.astype(jnp.int32)
    return jnp.where(kept, expert_ids * capacity + slot_rank, -1)


def exchange_dispatch(tokens, quantized, pair_weight, placement, ep_size, capacity):
    table = jnp.any(placement, axis=1).astype(jnp.bfloat16)
    bucket_shape = (ep_size, capacity, tokens.shape[1])
    send_x = contract_first(table, tokens).astype(jnp.bfloat16)
    send_q = contract_first(table, quantized).astype(jnp.bfloat16)
    send_weight = jnp.sum(jnp.where(placement, pair_weight[:, :, None], 0.0), axis=(0, 1))
    slot_x = exchange(send_x.reshape(bucket_shape), "ep").reshape(-1, tokens.shape[1])
    slot_q = exchange(send_q.reshape(bucket_shape), "ep").reshape(-1, tokens.shape[1])
    weight = exchange(send_weight.reshape(ep_size, capacity), "ep").reshape(-1)
    return slot_x, slot_q, weight


def relay_dispatch(tokens, quantized, target, pair_weight, capacity):
    ep_size, levels = lax.axis_size("ep"), lax.axis_size("ep") // 2
    me = lax.axis_index("ep")
    z, x = me // 2, me % 2
    meta = jnp.concatenate([target.astype(jnp.float32).T, pair_weight.T], axis=0)
    table = exchange(jnp.broadcast_to(meta[None], (ep_size, *meta.shape)), "ep")
    top = target.shape[1]
    slots = lax.broadcasted_iota(jnp.int32, (1, capacity, 1), 1).astype(jnp.float32)

    def hop(array, step, sign):
        sources = [h for h in range(levels) if 0 <= h - sign * (step - 1) < levels and 0 <= h + sign < levels]
        return lax.ppermute(
            array, "ep", [(2 * h + j, 2 * (h + sign) + j) for h in sources for j in range(2)]
        )

    def hit(block, expert):
        rows = lax.dynamic_index_in_dim(table, block, 0, keepdims=False)[:top]
        base = (expert * capacity).astype(jnp.float32)
        return jnp.any(rows[:, None, :] == slots + base, axis=0).astype(jnp.bfloat16)

    second = jnp.where(z == 0, 1, z - 1)
    third = jnp.where(z < 2, z + 2, z - 2)
    fourth = jnp.where(z == 0, 3, jnp.where(z == 1, 2, jnp.where(z == 2, 3, 0)))
    order = (z, second, third, fourth)
    own_hits = [hit(2 * h + x, me) for h in order]
    cross_hits = [hit(2 * h + x, me ^ 1) for h in order]
    inner = (z == 1) | (z == 2)

    def pick(hits, rows):
        return jnp.dot(hits, rows, preferred_element_type=jnp.float32).astype(jnp.bfloat16)

    def spread(block):
        up_one, down_one = hop(block, 1, 1), hop(block, 1, -1)
        up_two, down_two = hop(up_one, 2, 1), hop(down_one, 2, -1)
        up_three, down_three = hop(up_two, 3, 1), hop(down_two, 3, -1)
        held = (
            block,
            jnp.where(z == 0, down_one, up_one),
            jnp.where(z < 2, down_two, up_two),
            jnp.where(inner, down_one, jnp.where(z == 0, down_three, up_three)),
        )
        out = jnp.zeros((ep_size * capacity, block.shape[1]), jnp.bfloat16)
        for i in range(4):
            crossed = lax.ppermute(
                pick(cross_hits[i], held[i]), "ep", [(d, d ^ 1) for d in range(ep_size)]
            )
            kept_here = pick(own_hits[i], held[i])
            base = 2 * order[i]
            out = lax.dynamic_update_slice_in_dim(out, kept_here, (base + x) * capacity, 0)
            out = lax.dynamic_update_slice_in_dim(out, crossed, (base + 1 - x) * capacity, 0)
        return out, (up_one, down_one)

    slot_x, arrived = spread(tokens)
    quantized, _ = lax.optimization_barrier((quantized, arrived))
    slot_q, _ = spread(quantized)
    targets = table[:, :top, None, :]
    base = (me * capacity).astype(jnp.float32)
    weight = jnp.sum(
        jnp.where(targets == slots[None] + base, table[:, top:, None, :], 0.0), axis=(1, 3)
    )
    return slot_x, slot_q, weight.reshape(-1)


def exchange(array, axis):
    return lax.all_to_all(array, axis, split_axis=0, concat_axis=0, tiled=True)


def pair_scatter(deltas, values, after=None):
    dp_size = lax.axis_size("dp")
    hidden = deltas.shape[1]
    if dp_size != 4:
        part = contract_first(deltas, values).astype(jnp.bfloat16)
        return lax.psum_scatter(part, "dp", scatter_dimension=0, tiled=True), part
    share = hidden // dp_size
    me = lax.axis_index("dp")
    near, far = me ^ 1, me ^ 2

    def quarter(which):
        columns = lax.dynamic_slice_in_dim(deltas, which * share, share, 1)
        return contract_first(columns, values)

    def swap(array, bit):
        return lax.ppermute(array, "dp", [(i, i ^ bit) for i in range(dp_size)])

    from_near_far = swap(quarter(near ^ 2).astype(jnp.bfloat16), 1)
    from_near_own = swap(quarter(near).astype(jnp.bfloat16), 1)
    passed = (quarter(far) + from_near_far.astype(jnp.float32)).astype(jnp.bfloat16)
    from_far = swap(passed, 2)
    if after is not None:
        from_far, _ = lax.optimization_barrier((from_far, after))
    own = quarter(me) + from_near_own.astype(jnp.float32)
    return (own + from_far.astype(jnp.float32)).astype(jnp.bfloat16), passed


def on_device_body(
    grad_out, tokens, probs, expert_ids, priority, cap_counts, gate_weight, up_weight, down_weight
):
    ep_size = lax.axis_size("ep")
    tok_rows, model_width = tokens.shape
    route_count = expert_ids.shape[1]
    capacity = 5 * route_count * tok_rows // (4 * ep_size)
    slot_rows = ep_size * capacity
    bucket_shape = (ep_size, capacity, model_width)
    target = route_table(expert_ids, priority, cap_counts, ep_size, capacity)
    slot_range = lax.broadcasted_iota(jnp.int32, (1, 1, slot_rows), 2)
    placement = target[:, :, None] == slot_range
    row_scale = jnp.maximum(jnp.max(jnp.abs(grad_out), axis=1), 1.0)
    quantized = (grad_out / row_scale[:, None]).astype(jnp.bfloat16)
    pair_weight = probs * row_scale[:, None]
    if ep_size == 8:
        slot_x, slot_q, weight = relay_dispatch(tokens, quantized, target, pair_weight, capacity)
    else:
        slot_x, slot_q, weight = exchange_dispatch(
            tokens, quantized, pair_weight, placement, ep_size, capacity
        )
    weight = weight[:, None]
    w_gate = gate_weight[0]
    w_up = up_weight[0]
    w_down = down_weight[0]

    gate_pre = contract_last(slot_x, w_gate)
    up_pre = contract_last(slot_x, w_up)
    squash = jax.nn.sigmoid(sharpness * gate_pre)
    gated = gate_pre * squash
    activated = (up_pre + 1.0) * gated
    act_scaled = (activated * weight).astype(jnp.bfloat16)
    down_share, passed = pair_scatter(act_scaled, slot_q)
    later_q, _ = lax.optimization_barrier((slot_q, passed))
    back_proj = contract_last(later_q, w_down)
    act_delta = weight * back_proj
    up_delta = (act_delta * gated).astype(jnp.bfloat16)
    gate_delta = (
        act_delta * (up_pre + 1.0) * (squash + sharpness * gate_pre * squash * (1.0 - squash))
    ).astype(jnp.bfloat16)
    slot_out = jnp.sum(activated * back_proj, axis=1)
    gate_share, _ = pair_scatter(gate_delta, slot_x)
    up_share, _ = pair_scatter(up_delta, slot_x, gate_share)
    in_delta = jnp.dot(gate_delta, w_gate, preferred_element_type=jnp.float32) + jnp.dot(
        up_delta, w_up, preferred_element_type=jnp.float32
    )
    slot_in = in_delta.astype(jnp.bfloat16)
    back_in = exchange(slot_in.reshape(bucket_shape), "ep").reshape(slot_rows, model_width)
    back_prob = exchange(slot_out.reshape(ep_size, capacity), "ep").reshape(slot_rows)
    prob_grad = row_scale[:, None] * jnp.sum(
        jnp.where(placement, back_prob[None, None, :], 0.0), axis=2
    )
    table_low = jnp.any(placement, axis=1).astype(jnp.bfloat16)
    input_grad = jnp.dot(table_low, back_in, preferred_element_type=jnp.float32).astype(
        jnp.bfloat16
    )
    return (input_grad, prob_grad, gate_share[None], up_share[None], down_share[None])


MESH = pl.DeviceIdType.MESH


def fused_kernel(
    ep_size, dp_size, capacity, chunk,
    tokens_ref, grad_ref, probs_ref, ids_ref, prio_ref, caps_ref, gate_hbm, up_hbm, down_hbm,
    input_ref, prob_ref, grads_ref,
    w_gate, w_up, w_down, raw, slots, cross, deltas, act_part, weight_col,
    slot_sum, meta, target_col, scale_col, keep_out, keep_in, result, back, prob_out, prob_in,
    far_slots, far_deltas, far_weight, far_meta,
    load_sem, own_send, relay_send, raw_recv, cross_send, cross_recv, meta_send, meta_recv,
    keep_send, keep_recv, ret_send, ret_recv, prob_send, prob_recv,
    slot_send, slot_recv, side_send, side_recv, table_send, table_recv,
):
    tok_rows, width = tokens_ref.shape
    top = ids_ref.shape[0]
    hidden = w_gate.shape[0]
    share = hidden // dp_size
    chunks = width // chunk
    levels = ep_size // 2
    group = 2 * capacity
    pair = 2 * group
    units = 3
    me, rep = lax.axis_index("ep"), lax.axis_index("dp")
    z, x = lax.div(me, 2), lax.rem(me, 2)
    partner = me + 1 - 2 * x
    near = rep + 1 - 2 * lax.rem(rep, 2)
    far = lax.rem(rep + 2, dp_size)
    diagonal = lax.rem(near + 2, dp_size)
    high = lax.div(z, 2)
    middle = lax.div(z * (levels - 1 - z), 2)
    end = (levels - 1) * high
    first_target = middle * end + (1 - middle) * (1 + high)
    second_target = 2 - high

    def level_at(place):
        last = lax.div(place, 3)
        inner = lax.rem(place + 1, 3) * (1 - last) + 3 * last
        low = (1 - middle) * place + middle * inner
        return (1 - high) * low + high * (levels - 1 - low)

    def cols(index, size=chunk):
        return pl.ds(pl.multiple_of(index * size, size), size)

    def rows(index, size):
        return pl.ds(pl.multiple_of(index * size, size), size)

    def remote(source, target, send, recv, peer):
        return pltpu.make_async_remote_copy(
            src_ref=source, dst_ref=target, send_sem=send, recv_sem=recv,
            device_id=peer, device_id_type=MESH,
        )

    def raw_copy(tensor, level, index, target, sem):
        block = raw.at[tensor, level, index]
        return remote(block, block, sem, raw_recv.at[tensor, level, index], {"ep": 2 * target + x})

    def own_copy(tensor, which, index):
        target = first_target if which == 0 else second_target
        return raw_copy(tensor, z, index, target, own_send.at[tensor, which, index])

    def relay_copy(tensor, place, index):
        sem = relay_send.at[tensor, lax.div(place, 2), index]
        return raw_copy(tensor, level_at(place), index, end, sem)

    def cross_copy(tensor, place, index):
        return remote(
            cross.at[tensor, lax.rem(place, 2), index],
            slots.at[tensor, rows(2 * place + x, capacity), cols(index)],
            cross_send.at[tensor, place, index], cross_recv.at[tensor, place, index],
            {"ep": partner},
        )

    def meta_copy(step):
        peer = lax.rem(me + step, ep_size)
        return remote(meta.at[me], meta.at[me], meta_send.at[step], meta_recv.at[me], {"ep": peer})

    def meta_arrival(step):
        peer = lax.rem(me + step, ep_size)
        table = meta.at[peer]
        return remote(table, table, meta_send.at[step], meta_recv.at[peer], {"ep": peer})

    def table_copy(which):
        peer = far if which == 0 else diagonal
        return remote(
            meta, far_meta.at[which], table_send.at[which], table_recv.at[which], {"dp": peer}
        )

    def keep_copy(unit):
        return remote(
            keep_out.at[lax.rem(unit, 2)], keep_in.at[unit], keep_send.at[unit], keep_recv.at[unit],
            {"dp": near},
        )

    def far_rows(place, which):
        return pl.ds(pl.multiple_of(which * pair + lax.rem(place, 2) * group, group), group)

    def slot_copy(tensor, place, column):
        start = lax.rem(place, 2) * group + column * capacity
        return remote(
            slots.at[tensor, rows(2 * place + column, capacity)],
            far_slots.at[
                tensor, lax.div(place, 2), pl.ds(pl.multiple_of(start, capacity), capacity)
            ],
            slot_send.at[tensor, place, column], slot_recv.at[tensor, place, column], {"dp": far},
        )

    def side_copy(tensor, place):
        return remote(
            far_slots.at[tensor, lax.div(place, 2), far_rows(place, 0)],
            far_slots.at[tensor, lax.div(place, 2), far_rows(place, 1)],
            side_send.at[tensor, place], side_recv.at[tensor, place], {"dp": near},
        )

    def return_copy(place, column, block):
        return remote(
            result.at[rows(2 * place + column, capacity)], back.at[rows(me, capacity)],
            ret_send.at[place, column], ret_recv.at[me], {"ep": block},
        )

    def prob_copy(place, column, block):
        return remote(
            prob_out.at[place, column], prob_in.at[me],
            prob_send.at[place, column], prob_recv.at[me], {"ep": block},
        )

    def return_arrival(source):
        span = back.at[rows(source, capacity)]
        return remote(span, span, ret_send.at[0, 0], ret_recv.at[source], {"ep": source})

    def prob_arrival(source):
        span = prob_in.at[source]
        return remote(span, span, prob_send.at[0, 0], prob_recv.at[source], {"ep": source})

    loads = [
        pltpu.make_async_copy(source.at[0], target, load_sem.at[i])
        for i, (source, target) in enumerate(((gate_hbm, w_gate), (up_hbm, w_up), (down_hbm, w_down)))
    ]
    for load in loads:
        load.start()
    for index in range(chunks):
        raw[0, z, index] = tokens_ref[:, index * chunk : (index + 1) * chunk]

    barrier = pltpu.get_barrier_semaphore()
    for step in range(1, ep_size):
        pl.semaphore_signal(
            barrier, inc=1, device_id={"ep": lax.rem(me + step, ep_size)}, device_id_type=MESH
        )
    for peer in (near, far, diagonal):
        pl.semaphore_signal(barrier, inc=1, device_id={"dp": peer}, device_id_type=MESH)
    pl.semaphore_wait(barrier, ep_size + 2)

    own_copy(0, 0, 0).start()
    scale = jnp.maximum(jnp.max(jnp.abs(grad_ref[...]), axis=1, keepdims=True), 1.0)
    scale_col[...] = scale
    square = (tok_rows, tok_rows)
    eye = lax.broadcasted_iota(jnp.int32, square, 0) == lax.broadcasted_iota(jnp.int32, square, 1)

    def as_row(column):
        return jnp.sum(jnp.where(eye, column, 0.0), axis=0, keepdims=True)

    def as_column(row):
        return jnp.sum(jnp.where(eye, row, 0.0), axis=1, keepdims=True)

    prio_row = prio_ref[...].astype(jnp.float32)
    earlier = jnp.where(as_column(prio_row) < prio_row, 1.0, 0.0).astype(jnp.bfloat16)
    expert_iota = lax.broadcasted_iota(jnp.int32, (ep_size, tok_rows), 0)
    caps = jnp.zeros((ep_size, tok_rows), jnp.float32)
    for expert in range(ep_size):
        caps = jnp.where(expert_iota == expert, caps_ref[expert].astype(jnp.float32), caps)
    matches = [jnp.where(ids_ref[k : k + 1, :] == expert_iota, 1.0, 0.0) for k in range(top)]
    routed = sum(matches[1:], matches[0]).astype(jnp.bfloat16)
    before = jnp.dot(routed, earlier, preferred_element_type=jnp.float32)
    scale_row = as_row(scale)
    for k in range(top):
        rank = jnp.sum(matches[k] * before, axis=0, keepdims=True)
        limit = jnp.sum(matches[k] * caps, axis=0, keepdims=True)
        place = ids_ref[k : k + 1, :].astype(jnp.float32) * capacity + rank
        meta[me, k : k + 1, :] = jnp.where(rank < limit, place, -1.0)
        meta[me, top + k : top + k + 1, :] = probs_ref[k : k + 1, :] * scale_row
    for step in range(1, ep_size):
        meta_copy(step).start()
    for index in range(1, chunks):
        own_copy(0, 0, index).start()
    for index in range(chunks):
        piece = grad_ref[:, index * chunk : (index + 1) * chunk]
        raw[1, z, index] = (piece / scale).astype(jnp.bfloat16)
        own_copy(1, 0, index).start()
    for tensor in range(2):
        for index in range(chunks):
            own_copy(tensor, 1, index).start()
    for k in range(top):
        target_col[k] = as_column(meta[me, k : k + 1, :])

    slot_iota = lax.broadcasted_iota(jnp.int32, (capacity, tok_rows), 0)

    def slot_names(expert):
        return (slot_iota + expert * capacity).astype(jnp.float32)

    def hits(level, expert):
        table, names = meta[2 * level + x], slot_names(expert)
        total = jnp.zeros((capacity, tok_rows), jnp.float32)
        for k in range(top):
            total = total + jnp.where(table[k : k + 1] == names, 1.0, 0.0)
        return total.astype(jnp.bfloat16)

    def weight_of(table):
        names = slot_names(me)
        total = jnp.zeros((capacity, tok_rows), jnp.float32)
        for k in range(top):
            total = total + jnp.where(table[k : k + 1] == names, table[top + k : top + k + 1], 0.0)
        return jnp.sum(total, axis=1, keepdims=True)

    def event(tensor, place, index):
        level = level_at(place)

        @pl.when(place > 0)
        def _():
            raw_copy(tensor, level, index, end, relay_send.at[tensor, 0, index]).wait_recv()

        @pl.when(middle * lax.rem(place, 2) == 1)
        def _():
            relay_copy(tensor, place, index).start()

        @pl.when(place > 1)
        def _():
            cross_copy(tensor, place - 2, index).wait_send()

        block = raw[tensor, level, index]
        crossed = jnp.dot(hits(level, partner), block, preferred_element_type=jnp.float32)
        cross[tensor, lax.rem(place, 2), index] = crossed.astype(jnp.bfloat16)
        cross_copy(tensor, place, index).start()
        kept = jnp.dot(hits(level, me), block, preferred_element_type=jnp.float32)
        slots[tensor, rows(2 * place + x, capacity), cols(index)] = kept.astype(jnp.bfloat16)

        @pl.when(index == chunks - 1)
        def _():
            slot_copy(tensor, place, x).start()

    def share_slots(tensor, place):
        for index in range(chunks):
            cross_copy(tensor, place, index).wait_recv()
        slot_copy(tensor, place, 1 - x).start()

    def activate(gate_pre, up_pre):
        up_one = up_pre + 1.0
        squash = jax.nn.sigmoid(sharpness * gate_pre)
        gated = gate_pre * squash
        return gated, up_one * (squash + sharpness * gated * (1.0 - squash)), up_one * gated

    def forward_part(first, count, part):
        @pl.when(part == 0)
        def _():
            for inner in range(count):
                for column in range(2):
                    base = inner * group + column * capacity
                    table = meta[2 * level_at(first + inner) + column]
                    weight_col[base : base + capacity, :] = weight_of(table)

        size = count * group
        span = pl.ds(pl.multiple_of(first * group, group), size)
        entries = slots[0, span, :]
        gate_pre = contract_last(entries, w_gate[rows(part, chunk), :])
        up_pre = contract_last(entries, w_up[rows(part, chunk), :])
        gated, slope, activated = activate(gate_pre, up_pre)
        deltas[1, span, cols(part)] = slope.astype(jnp.bfloat16)
        deltas[2, span, cols(part)] = gated.astype(jnp.bfloat16)
        act_part[part, :size] = activated.astype(jnp.bfloat16)
        deltas[0, span, cols(part)] = (activated * weight_col[:size]).astype(jnp.bfloat16)

    def backward_part(first, count, part):
        size = count * group
        span = pl.ds(pl.multiple_of(first * group, group), size)
        back_proj = contract_last(slots[1, span, :], w_down[rows(part, chunk), :])
        act_delta = weight_col[:size] * back_proj
        for kind in (1, 2):
            stored = deltas[kind, span, cols(part)]
            deltas[kind, span, cols(part)] = (act_delta * stored).astype(jnp.bfloat16)
        slot_sum[part, :size] = jnp.sum(act_part[part, :size] * back_proj, axis=1, keepdims=True)

        @pl.when(part == chunks - 1)
        def _():
            total = slot_sum[0, :size]
            for other in range(1, chunks):
                total = total + slot_sum[other, :size]
            cap_square = (capacity, tok_rows)
            mask = lax.broadcasted_iota(jnp.int32, cap_square, 1) == slot_iota
            for inner in range(count):
                for column in range(2):
                    base = inner * group + column * capacity
                    line = jnp.sum(
                        jnp.where(mask, total[base : base + capacity], 0.0), axis=0, keepdims=True
                    )
                    prob_out[first + inner, column] = jnp.broadcast_to(line, prob_out.shape[2:])

    def return_part(first, count, part):
        span = pl.ds(pl.multiple_of(first * group, group), count * group)
        total = jnp.dot(
            deltas[1, span, :], w_gate[:, cols(part)], preferred_element_type=jnp.float32
        ) + jnp.dot(deltas[2, span, :], w_up[:, cols(part)], preferred_element_type=jnp.float32)
        result[span, cols(part)] = total.astype(jnp.bfloat16)

        @pl.when((part == chunks - 1) & ((first == 0) | (middle == 0)))
        def _():
            send_back(first, count)

    def send_back(first, count):
        for inner in range(count):
            place = first + count - 1 - inner
            for column in range(2):
                block = 2 * level_at(place) + column

                @pl.when(block != me)
                def _():
                    return_copy(place, column, block).start()
                    prob_copy(place, column, block).start()

                @pl.when(block == me)
                def _():
                    back[rows(me, capacity), :] = result[rows(2 * place + column, capacity), :]
                    prob_in[me] = prob_out[place, column]

    period = 4 * chunks

    def main_step(step, carry):
        @pl.when(step == 2 * chunks)
        def _():
            for hop in range(1, ep_size):
                meta_arrival(hop).wait_recv()
            for which in range(2):
                table_copy(which).start()
            for load in loads:
                load.wait()

        @pl.when(step < 2 * period)
        def _():
            item = lax.div(step, chunks)
            event(lax.rem(item, 2), lax.div(item, 2), lax.rem(step, chunks))

        late = step - chunks - 1

        @pl.when((late >= 0) & (lax.rem(late + period, chunks) == 0))
        def _():
            item = lax.div(late, chunks)

            @pl.when(item < 2 * levels)
            def _():
                share_slots(lax.rem(item, 2), lax.div(item, 2))

        for number, task in enumerate((forward_part, backward_part, return_part)):
            since = step - (3 + number) * chunks - 1

            @pl.when((since >= 0) & (lax.rem(since + 2 * period, period) < chunks))
            def _():
                task(2 * lax.div(since, period), 2, lax.rem(since, period))

        return carry

    lax.fori_loop(0, 2 * period + 2 * chunks + 1, main_step, 0)

    def keep_step(unit, carry):
        total = partial_of(unit, near).astype(jnp.bfloat16)

        @pl.when(unit >= 2)
        def _():
            keep_copy(unit - 2).wait_send()

        keep_out[lax.rem(unit, 2)] = total
        keep_copy(unit).start()
        return carry

    def partial_of(unit, quarter):
        return contract_first(deltas[unit, :, cols(quarter, share)], slots[1 - lax.div(unit + 1, 2)])

    def far_partial(unit, half):
        return contract_first(far_deltas[unit], far_slots[1 - lax.div(unit + 1, 2), half])

    def pull(tensor, half):
        for inner in range(2):
            for column in range(2):
                slot_copy(tensor, 2 * half + inner, column).wait_recv()
            side_copy(tensor, 2 * half + inner).start()

    def settle(tensor, half):
        for inner in range(2):
            side_copy(tensor, 2 * half + inner).wait_recv()

    def far_forward(half):
        for which in range(2):
            for inner in range(2):
                for column in range(2):
                    base = which * pair + inner * group + column * capacity
                    table = far_meta[which, 2 * level_at(2 * half + inner) + column]
                    far_weight[base : base + capacity, :] = weight_of(table)
        entries = far_slots[0, half]
        gate_pre = contract_last(entries, w_gate[rows(rep, share), :])
        up_pre = contract_last(entries, w_up[rows(rep, share), :])
        gated, slope, activated = activate(gate_pre, up_pre)
        far_deltas[1] = slope.astype(jnp.bfloat16)
        far_deltas[2] = gated.astype(jnp.bfloat16)
        far_deltas[0] = (activated * far_weight[...]).astype(jnp.bfloat16)

    def far_backward(half):
        back_proj = contract_last(far_slots[1, half], w_down[rows(rep, share), :])
        act_delta = far_weight[...] * back_proj
        for kind in (1, 2):
            far_deltas[kind] = (act_delta * far_deltas[kind]).astype(jnp.bfloat16)

    def combine():
        for step in range(1, ep_size):
            source = lax.rem(me + step, ep_size)
            return_arrival(source).wait_recv()
            prob_arrival(source).wait_recv()
        shape = (tok_rows, ep_size * capacity)
        names = lax.broadcasted_iota(jnp.int32, shape, 1).astype(jnp.float32)
        table = jnp.zeros(shape, jnp.float32)
        for k in range(top):
            table = table + jnp.where(target_col[k] == names, 1.0, 0.0)
        table = table.astype(jnp.bfloat16)
        for index in range(chunks):
            span = slice(index * chunk, (index + 1) * chunk)
            input_ref[:, span] = jnp.dot(
                table, back[:, span], preferred_element_type=jnp.float32
            ).astype(jnp.bfloat16)
        lane_name = lax.broadcasted_iota(jnp.int32, square, 1).astype(jnp.float32)
        for k in range(top):
            total = jnp.zeros((tok_rows, tok_rows), jnp.float32)
            for expert in range(ep_size):
                found = target_col[k] == lane_name + float(expert * capacity)
                total = total + jnp.where(found, prob_in[expert][:1], 0.0)
            prob_ref[k : k + 1, :] = as_row(scale_col[...] * jnp.sum(total, axis=1, keepdims=True))

    def far_step(half, carry):
        @pl.when(half == 0)
        def _():
            pull(0, 0)
            pull(1, 0)
            for which in range(2):
                table_copy(which).wait_recv()
            lax.fori_loop(0, units, keep_step, 0)

        settle(0, half)
        far_forward(half)

        settle(1, half)
        far_backward(half)

        @pl.when((half == 0) & (middle == 1))
        def _():
            send_back(2, 2)

        def grads_step(unit, inner):
            total = far_partial(unit, half)

            @pl.when((half == 0) & (unit > 0))
            def _():
                pull(unit - 1, 1)

            @pl.when(half == 0)
            def _():
                first = total + partial_of(unit, rep)
                keep_copy(unit).wait_recv()
                grads_ref[unit] = (first + keep_in[unit].astype(jnp.float32)).astype(jnp.bfloat16)

            @pl.when(half == 1)
            def _():
                grads_ref[unit] = (total + grads_ref[unit].astype(jnp.float32)).astype(jnp.bfloat16)

            return inner

        lax.fori_loop(0, units, grads_step, 0)
        return carry

    lax.fori_loop(0, 2, far_step, 0)
    combine()

    for tensor in range(2):
        for index in range(chunks):
            own_copy(tensor, 0, index).wait_send()
            own_copy(tensor, 1, index).wait_send()

            @pl.when(middle == 1)
            def _():
                relay_copy(tensor, 1, index).wait_send()
                relay_copy(tensor, 3, index).wait_send()

            for place in range(2, levels):
                cross_copy(tensor, place, index).wait_send()
        for place in range(levels):
            for column in range(2):
                slot_copy(tensor, place, column).wait_send()
            side_copy(tensor, place).wait_send()
    for step in range(1, ep_size):
        meta_copy(step).wait_send()
    for place in range(levels):
        for column in range(2):
            block = 2 * level_at(place) + column

            @pl.when(block != me)
            def _():
                return_copy(place, column, block).wait_send()
                prob_copy(place, column, block).wait_send()

    for step in (1, 2):
        keep_copy(units - step).wait_send()
    for which in range(2):
        table_copy(which).wait_send()


def emit_kernel(input_in, prob_in, grads_in, *refs):
    outs, (stage_input, stage_prob, stage_grads, load_sem, store_sem) = refs[:5], refs[5:]
    half = grads_in.shape[1] // 2
    moves = [(input_in, stage_input, outs[0]), (prob_in, stage_prob, outs[1])]
    for target, tensor in ((outs[2], 1), (outs[3], 2), (outs[4], 0)):
        for part in range(2):
            span = pl.ds(part * half, half)
            moves.append(
                (grads_in.at[tensor, span], stage_grads.at[tensor, span], target.at[0, span])
            )
    loads = [
        pltpu.make_async_copy(source, stage, load_sem.at[i])
        for i, (source, stage, _) in enumerate(moves)
    ]
    stores = [
        pltpu.make_async_copy(stage, target, store_sem.at[i])
        for i, (_, stage, target) in enumerate(moves)
    ]
    for load in loads:
        load.start()
    for load, store in zip(loads, stores):
        load.wait()
        store.start()
    for store in stores:
        store.wait()


def fused_body(
    grad_out, tokens, probs, expert_ids, priority, cap_counts, gate_weight, up_weight, down_weight
):
    ep_size, dp_size = lax.axis_size("ep"), lax.axis_size("dp")
    tok_rows, width = tokens.shape
    top = expert_ids.shape[1]
    hidden = gate_weight.shape[1]
    capacity = 5 * top * tok_rows // (4 * ep_size)
    slot_rows = ep_size * capacity
    pair = slot_rows // 2
    chunk = width // 3
    chunks, levels = width // chunk, ep_size // 2
    share = hidden // dp_size
    units = 3
    bf16, f32 = jnp.bfloat16, jnp.float32
    vmem, dma = pltpu.VMEM, pltpu.SemaphoreType.DMA
    in_vmem = pl.BlockSpec(memory_space=pltpu.VMEM)
    anywhere = pl.BlockSpec(memory_space=pl.ANY)
    scratch = [
        vmem((hidden, width), bf16), vmem((hidden, width), bf16), vmem((hidden, width), bf16),
        vmem((2, levels, chunks, tok_rows, chunk), bf16),
        vmem((2, slot_rows, width), bf16),
        vmem((2, 2, chunks, capacity, chunk), bf16),
        vmem((3, slot_rows, hidden), bf16),
        vmem((chunks, pair, chunk), bf16),
        vmem((pair, 1), f32),
        vmem((chunks, pair, 1), f32),
        vmem((ep_size, 2 * top, tok_rows), f32),
        vmem((top, tok_rows, 1), f32),
        vmem((tok_rows, 1), f32),
        vmem((2, share, width), bf16),
        vmem((units, share, width), bf16),
        vmem((slot_rows, width), bf16),
        vmem((slot_rows, width), bf16),
        vmem((levels, 2, 8, tok_rows), f32),
        vmem((ep_size, 8, tok_rows), f32),
        vmem((2, 2, 2 * pair, width), bf16),
        vmem((3, 2 * pair, share), bf16),
        vmem((2 * pair, 1), f32),
        vmem((2, ep_size, 2 * top, tok_rows), f32),
        dma((3,)), dma((2, 2, chunks)), dma((2, 2, chunks)), dma((2, levels, chunks)),
        dma((2, levels, chunks)), dma((2, levels, chunks)), dma((ep_size,)), dma((ep_size,)),
        dma((units,)), dma((units,)), dma((levels, 2)), dma((ep_size,)), dma((levels, 2)),
        dma((ep_size,)), dma((2, levels, 2)), dma((2, levels, 2)), dma((2, levels)), dma((2, levels)),
        dma((2,)), dma((2,)),
    ]
    input_grad, prob_grad, grads = pl.pallas_call(
        functools.partial(fused_kernel, ep_size, dp_size, capacity, chunk),
        out_shape=(
            jax.ShapeDtypeStruct((tok_rows, width), bf16),
            jax.ShapeDtypeStruct((top, tok_rows), f32),
            jax.ShapeDtypeStruct((3, share, width), bf16),
        ),
        in_specs=[in_vmem] * 5 + [pl.BlockSpec(memory_space=pltpu.SMEM)] + [anywhere] * 3,
        out_specs=(in_vmem, in_vmem, in_vmem),
        scratch_shapes=scratch,
        compiler_params=pltpu.CompilerParams(
            collective_id=0, has_side_effects=True, vmem_limit_bytes=66_000_000
        ),
        name="fused_step",
    )(
        tokens, grad_out, probs.T, expert_ids.T, priority, cap_counts, gate_weight, up_weight, down_weight
    )
    weight_shape = jax.ShapeDtypeStruct((1, share, width), bf16)
    outs = pl.pallas_call(
        emit_kernel,
        out_shape=(
            jax.ShapeDtypeStruct(input_grad.shape, bf16),
            jax.ShapeDtypeStruct(prob_grad.shape, f32),
            weight_shape, weight_shape, weight_shape,
        ),
        in_specs=[anywhere] * 3,
        out_specs=[anywhere] * 5,
        scratch_shapes=[
            vmem(input_grad.shape, bf16), vmem(prob_grad.shape, f32), vmem(grads.shape, bf16),
            dma((8,)), dma((8,)),
        ],
        name="emit",
    )(input_grad, prob_grad, grads)
    return outs[0], outs[1].T, outs[2], outs[3], outs[4]


def on_device(*arrays):
    return on_device_body(*arrays)


def solution(mesh):
    fused = mesh.shape["ep"] == 8 and mesh.shape["dp"] == 4
    return jax.shard_map(
        fused_body if fused else on_device,
        mesh=mesh,
        in_specs=(
            P(("ep", "dp"), None),
            P(("ep", "dp"), None),
            P(("ep", "dp"), None),
            P(("ep", "dp"), None),
            P(("ep", "dp"), None),
            P(),
            P("ep", None, None),
            P("ep", None, None),
            P("ep", None, None),
        ),
        out_specs=(
            P(("ep", "dp"), None),
            P(("ep", "dp"), None),
            P("ep", "dp", None),
            P("ep", "dp", None),
            P("ep", "dp", None),
        ),
        check_vma=False,
    )
```
